16 devices in a mesh: dp: 2 (over y, z), tp: 8 (over x, core).
Axes of the slice: x: 4, y: 2, z: 1, core: 2. Of those that a mesh axis runs over, the one named last changes fastest.
The devices are a block of a 4x4x8 slice.
Arguments:
- y_one: float32 [16, 256, 1408], P('dp'), parts along dimension 0
- y_two: float32 [16, 256, 1408], P('dp'), parts along dimension 0
- dy_one: float32 [16, 256, 1408], P('dp'), parts along dimension 0
- dy_two: float32 [16, 256, 1408], P('dp'), parts along dimension 0
- saved_one: float32 [1, 16, 256, 1408], P(None, 'dp'), parts along dimension 1
- saved_two: float32 [1, 16, 256, 1408], P(None, 'dp'), parts along dimension 1
- w_qkv: bfloat16 [3, 1408, 3, 16, 88], P(None, None, None, 'tp')
- w_o: bfloat16 [3, 16, 88, 1408], P(None, 'tp')
- w_in: bfloat16 [3, 1408, 6144], P(None, None, 'tp')
- w_out: bfloat16 [3, 6144, 1408], P(None, 'tp')
Outputs:
- output 1: float32 [16, 256, 1408], P('dp'), parts along dimension 0
- output 2: float32 [16, 256, 1408], P('dp'), parts along dimension 0
- output 3: float32 [16, 256, 1408], P('dp'), parts along dimension 0
- output 4: float32 [16, 256, 1408], P('dp'), parts along dimension 0
- output 5: float32 [6, 1408, 3, 16, 88], P('dp', None, None, 'tp'), parts along dimension 0
- output 6: float32 [6, 16, 88, 1408], P('dp', 'tp'), parts along dimension 0
- output 7: float32 [6, 1408, 6144], P('dp', None, 'tp'), parts along dimension 0
- output 8: float32 [6, 6144, 1408], P('dp', 'tp'), parts along dimension 0
There are 2 independent parts. The reference program is written for one: setup_inputs(seed, part) draws one part's arguments, and reference() takes and returns one part's arrays. A program takes and returns all parts, laid end to end along the dimension named above; an argument that names none is the same for every part.
All inputs are finite; a program needn't handle non-finite values.
Results may differ from the reference program's by a relative error of at most 0.012256.
Values are sent between devices in bfloat16 or wider.
A program may use at most 768 MiB of HBM per device.

```python
import jax
import jax.numpy as jnp
from jax import lax

SEQS = 8
SEQ = 256
HIDDEN = 1408
HEADS = 16
FF = 6144
PAIRS = 1

LAYERS = 2 * PAIRS + 1
HEAD = HIDDEN // HEADS
EPS = 1e-6


def setup_inputs(seed: int = 0, part: int = 0) -> dict:
    base_keys = jax.random.split(jax.random.key(seed), 2)
    act_keys = jax.random.split(jax.random.fold_in(base_keys[0], part), 6)
    w_keys = jax.random.split(base_keys[1], 4)
    state_shape = (SEQS, SEQ, HIDDEN)
    saved_shape = (PAIRS, SEQS, SEQ, HIDDEN)
    qk_gain = jnp.array([2.0 ** 0.5, 2.0 ** 0.5, 1.0], jnp.float32).reshape(1, 1, 3, 1, 1)
    wo_gain = 0.3 * (SEQ / 55.0) ** 0.5
    w_qkv = jax.random.normal(w_keys[0], (LAYERS, HIDDEN, 3, HEADS, HEAD), jnp.float32) * (HIDDEN ** -0.5) * qk_gain
    w_o = jax.random.normal(w_keys[1], (LAYERS, HEADS, HEAD, HIDDEN), jnp.float32) * (HIDDEN ** -0.5 * wo_gain)
    w_in = jax.random.normal(w_keys[2], (LAYERS, HIDDEN, FF), jnp.float32) * (HIDDEN ** -0.5)
    w_out = jax.random.normal(w_keys[3], (LAYERS, FF, HIDDEN), jnp.float32) * (0.45 * FF ** -0.5)
    return {
        "y_one": jax.random.normal(act_keys[0], state_shape, jnp.float32),
        "y_two": jax.random.normal(act_keys[1], state_shape, jnp.float32),
        "dy_one": jax.random.normal(act_keys[2], state_shape, jnp.float32),
        "dy_two": jax.random.normal(act_keys[3], state_shape, jnp.float32),
        "saved_one": jax.random.normal(act_keys[4], saved_shape, jnp.float32),
        "saved_two": jax.random.normal(act_keys[5], saved_shape, jnp.float32),
        "w_qkv": w_qkv.astype(jnp.bfloat16),
        "w_o": w_o.astype(jnp.bfloat16),
        "w_in": w_in.astype(jnp.bfloat16),
        "w_out": w_out.astype(jnp.bfloat16),
    }


def rms_norm(state):
    return state * lax.rsqrt(jnp.mean(state * state, axis=-1, keepdims=True) + EPS)


def to_bf(values):
    return values.astype(jnp.bfloat16).astype(jnp.float32)


def attend_one(qkv_one):
    q_one, k_one, v_one = qkv_one
    scores = jnp.einsum("qne,kne->nqk", q_one, k_one) * HEAD ** -0.5
    attn_probs = jax.nn.softmax(scores, axis=-1)
    return jnp.einsum("nqk,kne->qne", to_bf(attn_probs), v_one)


def branch_f(state, w_qkv, w_o):
    normed = to_bf(rms_norm(state))
    qkv_all = to_bf(jnp.einsum("bsh,hkne->kbsne", normed, w_qkv))
    heads_out = lax.map(jax.checkpoint(attend_one), (qkv_all[0], qkv_all[1], qkv_all[2]))
    return jnp.einsum("bsne,neh->bsh", to_bf(heads_out), w_o)


def branch_g(state, w_in, w_out):
    normed = to_bf(rms_norm(state))
    hidden = jnp.einsum("bsh,hf->bsf", normed, w_in)
    return jnp.einsum("bsf,fh->bsh", to_bf(jax.nn.gelu(hidden, approximate=True)), w_out)


def reversible_back(block_w, y_one, y_two, d_one, d_two):
    w_qkv, w_o, w_in, w_out = block_w
    g_val, g_pull = jax.vjp(branch_g, y_one, w_in, w_out)
    x_two = y_two - g_val
    g_dx, g_win, g_wout = g_pull(d_two)
    d_one = d_one + g_dx
    f_val, f_pull = jax.vjp(branch_f, x_two, w_qkv, w_o)
    x_one = y_one - f_val
    f_dx, f_wqkv, f_wo = f_pull(d_one)
    return x_one, x_two, d_one, d_two + f_dx, (f_wqkv, f_wo, g_win, g_wout)


def plain_back(block_w, x_one, x_two, d_one, d_two):
    w_qkv, w_o, w_in, w_out = block_w
    f_pull = jax.vjp(branch_f, x_two, w_qkv, w_o)[1]
    f_dx, f_wqkv, f_wo = f_pull(d_one)
    g_pull = jax.vjp(branch_g, x_one, w_in, w_out)[1]
    g_dx, g_win, g_wout = g_pull(d_two)
    return d_one + g_dx, d_two + f_dx, (f_wqkv, f_wo, g_win, g_wout)


def reference(y_one, y_two, dy_one, dy_two, saved_one, saved_two, w_qkv, w_o, w_in, w_out):
    weights = tuple(weight.astype(jnp.float32) for weight in (w_qkv, w_o, w_in, w_out))
    top_w = tuple(weight[LAYERS - 1] for weight in weights)
    x_one, x_two, d_one, d_two, top_grads = reversible_back(top_w, y_one, y_two, dy_one, dy_two)
    paired = tuple(weight[: 2 * PAIRS].reshape((PAIRS, 2) + weight.shape[1:]) for weight in weights)
    rev_w = tuple(weight[:, 0] for weight in paired)
    plain_w = tuple(weight[:, 1] for weight in paired)

    def pair_step(carry_in, scan_in):
        rev_block_w, plain_block_w, s_one, s_two = scan_in
        d_mid_one, d_mid_two, plain_grads = plain_back(plain_block_w, s_one, s_two, carry_in[2], carry_in[3])
        carry_out = reversible_back(rev_block_w, s_one, s_two, d_mid_one, d_mid_two)
        return carry_out[:4], (carry_out[4], plain_grads)

    final_state, scan_grads = lax.scan(pair_step, (x_one, x_two, d_one, d_two), (rev_w, plain_w, saved_one, saved_two), reverse=True)
    grad_out = tuple(
        jnp.concatenate([jnp.stack([rev_g, plain_g], axis=1).reshape((2 * PAIRS,) + rev_g.shape[1:]), top_g[None]], axis=0)
        for rev_g, plain_g, top_g in zip(scan_grads[0], scan_grads[1], top_grads)
    )
    return (final_state[0], final_state[1], final_state[2], final_state[3], grad_out[0], grad_out[1], grad_out[2], grad_out[3])
```

```python
import jax
import jax.numpy as jnp
from jax import lax
from jax.sharding import PartitionSpec as P

EPS = 1e-6
F32, BF16 = jnp.float32, jnp.bfloat16


def rms_scale(state):
    return lax.rsqrt(jnp.mean(state * state, axis=-1, keepdims=True) + EPS)


def rms_bf(state):
    return (state * rms_scale(state)).astype(BF16)


def rms_pull(state, cot):
    scale = rms_scale(state)
    normed = state * scale
    return scale * (cot - normed * jnp.mean(normed * cot, axis=-1, keepdims=True))


def gelu_tanh(hidden):
    return jax.nn.gelu(hidden, approximate=True)


def attn_forward(normed, w_qkv):
    head_dim = w_qkv.shape[-1]
    qkv_all = jnp.einsum("bsh,hkne->kbsne", normed, w_qkv, preferred_element_type=F32).astype(BF16)
    scores = jnp.einsum("bqne,bkne->bnqk", qkv_all[0], qkv_all[1], preferred_element_type=F32) * head_dim ** -0.5
    attn_probs = jax.nn.softmax(scores, axis=-1)
    probs_bf = attn_probs.astype(BF16)
    heads_out = jnp.einsum("bnqk,bkne->bqne", probs_bf, qkv_all[2], preferred_element_type=F32).astype(BF16)
    return qkv_all, attn_probs, probs_bf, heads_out


def attn_backward(normed, w_qkv, w_o, attn_cache, d_bf):
    qkv_all, attn_probs, probs_bf, heads_out = attn_cache
    head_dim = w_qkv.shape[-1]
    d_wo = jnp.einsum("bqne,bqh->neh", heads_out, d_bf, preferred_element_type=F32)
    d_heads = jnp.einsum("bqh,neh->bqne", d_bf, w_o, preferred_element_type=F32).astype(BF16)
    d_v = jnp.einsum("bnqk,bqne->bkne", probs_bf, d_heads, preferred_element_type=F32)
    d_probs = jnp.einsum("bqne,bkne->bnqk", d_heads, qkv_all[2], preferred_element_type=F32)
    d_scores = attn_probs * (d_probs - jnp.sum(d_probs * attn_probs, axis=-1, keepdims=True)) * head_dim ** -0.5
    ds_bf = d_scores.astype(BF16)
    d_q = jnp.einsum("bnqk,bkne->bqne", ds_bf, qkv_all[1], preferred_element_type=F32)
    d_k = jnp.einsum("bnqk,bqne->bkne", ds_bf, qkv_all[0], preferred_element_type=F32)
    d_qkv = jnp.stack([d_q.astype(BF16), d_k.astype(BF16), d_v.astype(BF16)], axis=2)
    d_normed = jnp.einsum("bskne,hkne->bsh", d_qkv, w_qkv, preferred_element_type=F32)
    d_wqkv = jnp.einsum("bsh,bskne->hkne", normed, d_qkv, preferred_element_type=F32)
    return d_normed, d_wqkv, d_wo


def mlp_forward(normed, w_in):
    hidden = jnp.einsum("bsh,hf->bsf", normed, w_in, preferred_element_type=F32)
    gelu_out, gelu_pull = jax.vjp(gelu_tanh, hidden)
    return gelu_out.astype(BF16), gelu_pull


def mlp_backward(normed, w_in, w_out, act_bf, gelu_pull, d_bf):
    d_act = jnp.einsum("bsh,fh->bsf", d_bf, w_out, preferred_element_type=F32)
    d_hidden = gelu_pull(d_act)[0].astype(BF16)
    d_normed = jnp.einsum("bsf,hf->bsh", d_hidden, w_in, preferred_element_type=F32)
    d_wout = jnp.einsum("bsf,bsh->fh", act_bf, d_bf, preferred_element_type=F32)
    d_win = jnp.einsum("bsh,bsf->hf", normed, d_hidden, preferred_element_type=F32)
    return d_normed, d_win, d_wout


def scatter(part):
    return lax.psum_scatter(part, "tp", scatter_dimension=0, tiled=True)


def gather(shard):
    return lax.all_gather(shard, "tp", axis=0, tiled=True)


def solution(mesh):
    act_spec = P("dp", None, None)
    saved_spec = P(None, "dp", None, None)
    weight_specs = (P(None, None, None, "tp", None), P(None, "tp", None, None), P(None, None, "tp"), P(None, "tp", None))
    grad_specs = (P("dp", None, None, "tp", None), P("dp", "tp", None, None), P("dp", None, "tp"), P("dp", "tp", None))
    n_tp = mesh.shape["tp"]

    def per_device(y_one, y_two, dy_one, dy_two, saved_one, saved_two, w_qkv, w_o, w_in, w_out):
        n_layers = w_qkv.shape[0]
        n_pairs = saved_one.shape[0]
        rows = y_one.shape[0] // n_tp
        start = lax.axis_index("tp") * rows

        def own(state):
            return lax.dynamic_slice_in_dim(state, start, rows, 0)

        grads = [None] * n_layers

        top = n_layers - 1
        a_one = rms_bf(y_one)
        act, pull = mlp_forward(a_one, w_in[top])
        g_shard = scatter(jnp.einsum("bsf,fh->bsh", act, w_out[top], preferred_element_type=F32))
        d_two_bf = dy_two.astype(BF16)
        g_back, d_win, d_wout = mlp_backward(a_one, w_in[top], w_out[top], act, pull, d_two_bf)
        d_one = own(dy_one) + rms_pull(own(y_one), scatter(g_back.astype(BF16)).astype(F32))
        d_one_bf = gather(d_one.astype(BF16))
        x_two = own(y_two) - g_shard
        d_two = own(dy_two)
        f_in = gather(rms_bf(x_two))
        cache = attn_forward(f_in, w_qkv[top])
        f_back, d_wqkv, d_wo = attn_backward(f_in, w_qkv[top], w_o[top], cache, d_one_bf)
        d_two = d_two + rms_pull(x_two, scatter(f_back.astype(BF16)).astype(F32))
        grads[top] = (d_wqkv, d_wo, d_win, d_wout)

        for pair in reversed(range(n_pairs)):
            s_one, s_two = saved_one[pair], saved_two[pair]
            mid, low = 2 * pair + 1, 2 * pair
            a_one, a_two = rms_bf(s_one), rms_bf(s_two)
            d_two_bf = gather(d_two.astype(BF16))
            cache = attn_forward(a_two, w_qkv[mid])
            f_back, d_wqkv, d_wo = attn_backward(a_two, w_qkv[mid], w_o[mid], cache, d_one_bf)
            act, pull = mlp_forward(a_one, w_in[mid])
            g_back_mid, d_win, d_wout = mlp_backward(a_one, w_in[mid], w_out[mid], act, pull, d_two_bf)
            grads[mid] = (d_wqkv, d_wo, d_win, d_wout)
            d_two = d_two + rms_pull(own(s_two), scatter(f_back.astype(BF16)).astype(F32))
            d_two_bf = gather(d_two.astype(BF16))
            act, pull = mlp_forward(a_one, w_in[low])
            g_shard = scatter(jnp.einsum("bsf,fh->bsh", act, w_out[low], preferred_element_type=F32))
            x_two_shard = own(s_two) - g_shard
            x_two = gather(x_two_shard)
            f_in = rms_bf(x_two)
            cache = attn_forward(f_in, w_qkv[low])
            heads = cache[3]
            n_b, n_s, n_h, n_e = heads.shape
            heads_t = jnp.transpose(heads, (2, 3, 0, 1)).reshape(n_h * n_e, n_b * n_s)
            heads_all = gather(heads_t)
            wo_all = gather(w_o[low].reshape(n_h * n_e, -1))
            f_val = jnp.einsum("et,eh->th", heads_all, wo_all, preferred_element_type=F32)
            x_one = s_one - f_val.reshape(s_one.shape)
            g_back_low, d_win, d_wout = mlp_backward(a_one, w_in[low], w_out[low], act, pull, d_two_bf)
            g_back = scatter((g_back_mid + g_back_low).astype(BF16)).astype(F32)
            d_one = d_one + rms_pull(own(s_one), g_back)
            if pair == 0:
                d_one_full = gather(d_one)
                d_one_bf = d_one_full.astype(BF16)
            else:
                d_one_bf = gather(d_one.astype(BF16))
            f_back, d_wqkv, d_wo = attn_backward(f_in, w_qkv[low], w_o[low], cache, d_one_bf)
            d_two = d_two + rms_pull(x_two_shard, scatter(f_back.astype(BF16)).astype(F32))
            grads[low] = (d_wqkv, d_wo, d_win, d_wout)
        d_two_full = gather(d_two)
        stacked = tuple(jnp.stack([entry[slot] for entry in grads]) for slot in range(4))
        return (x_one, x_two, d_one_full, d_two_full) + stacked

    return jax.shard_map(
        per_device,
        mesh=mesh,
        in_specs=(act_spec,) * 4 + (saved_spec,) * 2 + weight_specs,
        out_specs=(act_spec,) * 4 + grad_specs,
        check_vma=False,
    )
```

```python
import functools

import jax
import jax.numpy as jnp
from jax import lax
from jax.experimental import pallas as pl
from jax.experimental.pallas import tpu as pltpu
from jax.sharding import PartitionSpec as P

EPS = 1e-6
F32, BF16 = jnp.float32, jnp.bfloat16
CORES = 2
VMEM = 60 * 1024 * 1024


def dot(lhs, rhs, lhs_dim, rhs_dim):
    return lax.dot_general(lhs, rhs, (((lhs_dim,), (rhs_dim,)), ((), ())), preferred_element_type=F32)


def later(value, *others):
    return lax.optimization_barrier((value,) + others)[0]


def rms_scale(state):
    return lax.rsqrt(jnp.mean(state * state, axis=-1, keepdims=True) + EPS)


def rms_bf(state):
    return (state * rms_scale(state)).astype(BF16)


def rms_pull(state, cot):
    scale = rms_scale(state)
    normed = state * scale
    return scale * (cot - normed * jnp.mean(normed * cot, axis=-1, keepdims=True))


class Plan:
    def __init__(self, core, n_seq):
        self.core = core
        self.n_seq = n_seq
        self.half = n_seq // CORES

    def after(self, *values):
        return Plan(later(self.core, *values), self.n_seq)

    def seq(self, g, core):
        far = g < self.half
        return CORES * lax.rem(g, self.half) + jnp.where(far, 1 - core[0], core[0])

    def whole(self, rows, cols):
        return pl.BlockSpec((1, rows, cols), lambda g, core: (self.seq(g, core), 0, 0))

    def step(self, rows, cols):
        return pl.BlockSpec((1, rows, cols), lambda g, core: (g, 0, 0))

    def far(self, rows, cols):
        return pl.BlockSpec((1, rows, cols), lambda g, core: (jnp.minimum(g, self.half - 1), 0, 0))

    def near(self, rows, cols):
        return pl.BlockSpec((1, rows, cols), lambda g, core: (jnp.maximum(g - self.half, 0), 0, 0))

    def pair(self, rows, cols):
        return [self.far(rows, cols), self.near(rows, cols)]

    def pair_shape(self, rows, cols, dtype):
        return [jax.ShapeDtypeStruct((self.half, rows, cols), dtype)] * CORES

    @staticmethod
    def layer(index, rows, cols):
        return pl.BlockSpec((1, rows, cols), lambda g, core: (index, 0, 0))

    def call(self, body, name, in_specs, out_specs, out_shape, args, flops, aliases=None):
        n_bytes = sum(x.size * x.dtype.itemsize for x in out_shape)
        return pl.pallas_call(
            body,
            name=name,
            grid_spec=pltpu.PrefetchScalarGridSpec(
                num_scalar_prefetch=1, grid=(self.n_seq,), in_specs=in_specs, out_specs=out_specs
            ),
            out_shape=out_shape,
            input_output_aliases=aliases or {},
            cost_estimate=pl.CostEstimate(flops=int(flops), bytes_accessed=int(n_bytes), transcendentals=0),
            compiler_params=pltpu.CompilerParams(dimension_semantics=("arbitrary",), vmem_limit_bytes=VMEM),
        )(self.core, *args)


def put_pair(half, far_ref, near_ref, value):
    g = pl.program_id(0)

    @pl.when(g < half)
    def _():
        far_ref[0] = value.astype(far_ref.dtype)

    @pl.when(g >= half)
    def _():
        near_ref[0] = value.astype(near_ref.dtype)


def get_pair(half, far_ref, near_ref):
    return jnp.where(pl.program_id(0) < half, far_ref[0], near_ref[0])


def gelu_parts(hidden):
    root = (2.0 / jnp.pi) ** 0.5
    square = hidden * hidden
    bent = jnp.tanh(root * (hidden + 0.044715 * (square * hidden)))
    cdf = 0.5 * (1.0 + bent)
    return hidden * cdf, bent, cdf, root, square


def mlp_forward(plan, state, w_in, w_out, layer):
    n_seq, rows, width = state.shape
    ff = w_in.shape[-1]

    def body(core, x_ref, win_ref, wout_ref, far_ref, near_ref):
        normed = rms_bf(x_ref[0])
        act = gelu_parts(dot(normed, win_ref[0], 1, 0))[0].astype(BF16)
        put_pair(plan.half, far_ref, near_ref, dot(act, wout_ref[0], 1, 0))

    return plan.call(
        body,
        "mlp_forward",
        [plan.whole(rows, width), plan.layer(layer, width, ff), plan.layer(layer, ff, width)],
        plan.pair(rows, width),
        plan.pair_shape(rows, width, F32),
        (state, w_in, w_out),
        4 * n_seq * rows * width * ff,
    )


def mlp_back(plan, state, d_out, w_in, w_out, layer, extra=None):
    n_seq, rows, width = state.shape
    ff = w_in.shape[-1]
    split_d = isinstance(d_out, (list, tuple))
    n_d, n_e = (CORES if split_d else 1), (CORES if extra is not None else 0)

    def body(core, x_ref, *refs):
        d_refs, e_refs, refs = refs[:n_d], refs[n_d : n_d + n_e], refs[n_d + n_e :]
        win_ref, wout_ref, dx_far, dx_near, a_ref, act_ref, dh_ref = refs
        normed = rms_bf(x_ref[0])
        d_bf = get_pair(plan.half, *d_refs) if split_d else d_refs[0][0].astype(BF16)
        hidden = dot(normed, win_ref[0], 1, 0)
        d_act = dot(d_bf, wout_ref[0], 1, 1)
        act, bent, cdf, root, square = gelu_parts(hidden)
        act = act.astype(BF16)
        slope = cdf + 0.5 * hidden * (1.0 - bent * bent) * (root * (1.0 + 3.0 * 0.044715 * square))
        d_hidden = (slope * d_act).astype(BF16)
        d_x = dot(d_hidden, win_ref[0], 1, 1)
        if n_e:
            d_x = d_x + get_pair(plan.half, *e_refs).astype(F32)
        put_pair(plan.half, dx_far, dx_near, d_x)
        a_ref[0] = normed
        act_ref[0] = act
        dh_ref[0] = d_hidden

    in_specs = [plan.whole(rows, width)]
    in_specs += plan.pair(rows, width) if split_d else [plan.whole(rows, width)]
    args = [state] + (list(d_out) if split_d else [d_out])
    if n_e:
        in_specs += plan.pair(rows, width)
        args += list(extra)
    in_specs += [plan.layer(layer, width, ff), plan.layer(layer, ff, width)]
    args += [w_in, w_out]
    out_specs = plan.pair(rows, width) + [plan.step(rows, width), plan.step(rows, ff), plan.step(rows, ff)]
    out_shape = plan.pair_shape(rows, width, BF16) + [
        jax.ShapeDtypeStruct((n_seq, rows, width), BF16),
        jax.ShapeDtypeStruct((n_seq, rows, ff), BF16),
        jax.ShapeDtypeStruct((n_seq, rows, ff), BF16),
    ]
    outs = plan.call(body, "mlp_back", in_specs, out_specs, out_shape, args, 6 * n_seq * rows * width * ff)
    return tuple(outs[:2]), tuple(outs[2:])


def mlp_grads(plan, parts, d_out, layer, n_layers, held):
    normed, act, d_hidden = parts
    n_seq, rows, width = normed.shape
    ff = act.shape[-1]
    split_d = isinstance(d_out, (list, tuple))
    n_d = CORES if split_d else 1
    n_held = 0 if held is None else 2

    def body(core, a_ref, act_ref, dh_ref, *refs):
        d_refs, (dwin_ref, dwout_ref) = refs[:n_d], refs[n_d + n_held :]
        d_bf = get_pair(plan.half, *d_refs) if split_d else d_refs[0][0].astype(BF16)
        d_win = dot(a_ref[0], dh_ref[0], 0, 0)
        d_wout = dot(act_ref[0], d_bf, 0, 0)

        @pl.when(pl.program_id(0) == 0)
        def _():
            dwin_ref[0] = d_win
            dwout_ref[0] = d_wout

        @pl.when(pl.program_id(0) > 0)
        def _():
            dwin_ref[0] += d_win
            dwout_ref[0] += d_wout

    in_specs = [plan.step(rows, width), plan.step(rows, ff), plan.step(rows, ff)]
    in_specs += plan.pair(rows, width) if split_d else [plan.whole(rows, width)]
    args = [normed, act, d_hidden] + (list(d_out) if split_d else [d_out])
    aliases = {}
    if n_held:
        aliases = {len(args) + 1 + i: i for i in range(n_held)}
        in_specs += [pl.BlockSpec(memory_space=pl.ANY)] * n_held
        args += list(held)
    return plan.call(
        body,
        "mlp_grads",
        in_specs,
        [plan.layer(layer, width, ff), plan.layer(layer, ff, width)],
        [jax.ShapeDtypeStruct((n_layers, width, ff), F32), jax.ShapeDtypeStruct((n_layers, ff, width), F32)],
        args,
        4 * n_seq * rows * width * ff,
        aliases,
    )


def softmax(scores):
    powers = jnp.exp(scores - jnp.max(scores, axis=-1, keepdims=True))
    return powers / jnp.sum(powers, axis=-1, keepdims=True)


def attn_forward(plan, state, w_t, layer, n_heads):
    rows, width = state[0].shape[-2:]
    n_seq, depth = plan.n_seq, w_t.shape[1]
    size = depth // 3 // n_heads

    def body(core, far_ref, near_ref, w_ref, out_ref, state_ref):
        x = get_pair(plan.half, far_ref, near_ref)
        state_ref[0] = x
        qkv = dot(w_ref[0], rms_bf(x), 1, 1)
        outs = []
        for head in range(n_heads):
            q, k, v = (qkv[(kind * n_heads + head) * size :][:size].astype(BF16) for kind in range(3))
            probs = softmax(dot(q, k, 0, 0) * size ** -0.5).astype(BF16)
            outs.append(dot(v, probs, 1, 1))
        out_ref[...] = jnp.concatenate(outs, axis=0).astype(BF16)

    return plan.call(
        body,
        "attn_forward",
        plan.pair(rows, width) + [plan.layer(layer, depth, width)],
        [pl.BlockSpec((depth // 3, rows), lambda g, core: (0, plan.seq(g, core))), plan.whole(rows, width)],
        [jax.ShapeDtypeStruct((depth // 3, n_seq * rows), BF16), jax.ShapeDtypeStruct((n_seq, rows, width), F32)],
        (*state, w_t),
        2 * n_seq * rows * width * depth,
    )


def attn_back(plan, state, d_out, w_t, w_o, layer, n_heads, n_layers, held, keep_d=False):
    split_x = isinstance(state, (list, tuple))
    split_d = isinstance(d_out, (list, tuple))
    rows, width = (state[0] if split_x else state).shape[-2:]
    n_seq, depth = plan.n_seq, w_t.shape[1]
    size = depth // 3 // n_heads
    n_x, n_d = (CORES if split_x else 1), (CORES if split_d else 1)
    n_held = 0 if held is None else 2

    def body(core, *refs):
        x_refs, d_refs, refs = refs[:n_x], refs[n_x : n_x + n_d], refs[n_x + n_d :]
        w_ref, wo_ref = refs[:2]
        dx_far, dx_near, dw_ref, dwo_ref = refs[2 + n_held :][:4]
        normed = get_pair(plan.half, *x_refs) if split_x else rms_bf(x_refs[0][0])
        d_all = get_pair(plan.half, *d_refs) if split_d else d_refs[0][0]
        d_bf = d_all.astype(BF16)
        if keep_d:
            refs[-1][0] = d_all
        qkv = dot(w_ref[0], normed, 1, 1)
        d_heads = dot(wo_ref[0], d_bf, 1, 1)
        outs, d_parts = [], [[], [], []]
        for head in range(n_heads):
            q, k, v = (qkv[(kind * n_heads + head) * size :][:size].astype(BF16) for kind in range(3))
            d_head = d_heads[head * size :][:size].astype(BF16)
            probs = softmax(dot(q, k, 0, 0) * size ** -0.5)
            probs_bf = probs.astype(BF16)
            outs.append(dot(v, probs_bf, 1, 1))
            d_probs = dot(d_head, v, 0, 0)
            d_scores = probs * (d_probs - jnp.sum(d_probs * probs, axis=-1, keepdims=True)) * size ** -0.5
            d_scores = d_scores.astype(BF16)
            d_parts[0].append(dot(k, d_scores, 1, 1))
            d_parts[1].append(dot(q, d_scores, 1, 0))
            d_parts[2].append(dot(d_head, probs_bf, 1, 0))
        d_qkv = jnp.concatenate(d_parts[0] + d_parts[1] + d_parts[2], axis=0).astype(BF16)
        put_pair(plan.half, dx_far, dx_near, dot(d_qkv, w_ref[0], 0, 0))
        d_w = dot(d_qkv, normed, 1, 0)
        d_wo = dot(jnp.concatenate(outs, axis=0).astype(BF16), d_bf, 1, 0)

        @pl.when(pl.program_id(0) == 0)
        def _():
            dw_ref[0] = d_w
            dwo_ref[0] = d_wo

        @pl.when(pl.program_id(0) > 0)
        def _():
            dw_ref[0] += d_w
            dwo_ref[0] += d_wo

    in_specs = plan.pair(rows, width) if split_x else [plan.whole(rows, width)]
    in_specs = in_specs + (plan.pair(rows, width) if split_d else [plan.whole(rows, width)])
    in_specs += [plan.layer(layer, depth, width), plan.layer(layer, depth // 3, width)]
    args = (list(state) if split_x else [state]) + (list(d_out) if split_d else [d_out]) + [w_t, w_o]
    aliases = {}
    if n_held:
        aliases = {len(args) + 1 + i: CORES + i for i in range(n_held)}
        in_specs += [pl.BlockSpec(memory_space=pl.ANY)] * n_held
        args += list(held)
    out_specs = plan.pair(rows, width) + [plan.layer(layer, depth, width), plan.layer(layer, depth // 3, width)]
    out_shape = plan.pair_shape(rows, width, BF16)
    out_shape += [jax.ShapeDtypeStruct((n_layers, depth, width), F32), jax.ShapeDtypeStruct((n_layers, depth // 3, width), F32)]
    if keep_d:
        out_specs.append(plan.whole(rows, width))
        out_shape.append(jax.ShapeDtypeStruct((n_seq, rows, width), F32))
    outs = plan.call(body, "attn_back", in_specs, out_specs, out_shape, args, 8 * n_seq * rows * width * depth, aliases)
    return tuple(outs[:2]), tuple(outs[2:4]), (outs[4] if keep_d else None)


def in_order(plan, pair):
    rows, width = pair[0].shape[-2:]

    def body(core, far_ref, near_ref, out_ref):
        out_ref[0] = get_pair(plan.half, far_ref, near_ref)

    shape = jax.ShapeDtypeStruct((plan.n_seq, rows, width), pair[0].dtype)
    specs = plan.pair(rows, width)
    return plan.call(body, "in_order", specs, [plan.whole(rows, width)], [shape], pair, plan.n_seq * rows * width)[0]


def project_out(plan, base, heads, w_o):
    n_seq, rows, width = base.shape
    depth = heads[0].shape[0]

    def body(core, x_ref, h0_ref, h1_ref, w0_ref, w1_ref, out_ref):
        total = dot(h0_ref[...], w0_ref[...], 0, 0) + dot(h1_ref[...], w1_ref[...], 0, 0)
        out_ref[0] = x_ref[0] - total

    head_spec = pl.BlockSpec((depth, rows), lambda g, core: (0, g))
    w_spec = pl.BlockSpec((depth, width), lambda g, core: (0, 0))
    return plan.call(
        body,
        "project_out",
        [plan.step(rows, width), head_spec, head_spec, w_spec, w_spec],
        [plan.step(rows, width)],
        [jax.ShapeDtypeStruct(base.shape, F32)],
        (base, *heads, *w_o),
        4 * n_seq * rows * width * depth,
    )[0]


def solution(mesh):
    act_spec = P("dp", None, None)
    saved_spec = P(None, "dp", None, None)
    weight_specs = (P(None, None, None, "tp", None), P(None, "tp", None, None), P(None, None, "tp"), P(None, "tp", None))
    grad_specs = (P("dp", None, None, "tp", None), P("dp", "tp", None, None), P("dp", None, "tp"), P("dp", "tp", None))
    n_tp = mesh.shape["tp"]
    alike = [list(range(core, n_tp, CORES)) for core in range(CORES)]
    partners = [(i, i + 1 - 2 * (i % CORES)) for i in range(n_tp)]

    def swap(value):
        return lax.ppermute(value, "tp", partners)

    def scatter(pair):
        far, near = pair
        both = near.astype(F32) + swap(far).astype(F32)
        return lax.psum_scatter(both.astype(far.dtype), "tp", scatter_dimension=0, axis_index_groups=alike, tiled=True)

    def gather(shard, *others):
        near = lax.all_gather(shard, "tp", axis=0, axis_index_groups=alike, tiled=True)
        near = later(near, *others)
        return swap(near), near

    def per_device(y_one, y_two, dy_one, dy_two, saved_one, saved_two, w_qkv, w_o, w_in, w_out):
        n_layers, width, _, n_heads, size = w_qkv.shape
        n_pairs = saved_one.shape[0]
        me = lax.axis_index("tp")
        core = lax.rem(me, CORES)
        plan = Plan(core.reshape(1).astype(jnp.int32), y_one.shape[0])
        w_t = jnp.transpose(w_qkv, (0, 2, 3, 4, 1)).reshape(n_layers, 3 * n_heads * size, width)
        w_o2 = w_o.reshape(n_layers, n_heads * size, width)

        def own(state):
            return lax.dynamic_slice_in_dim(state, me, 1, 0)

        wo_low = gather(w_o2[0])
        top = n_layers - 1
        dx_pair, parts = mlp_back(plan, y_one, dy_two, w_in, w_out, top)
        g_back = scatter(dx_pair)
        g_top = mlp_forward(plan.after(dx_pair[0], wo_low[1]), y_one, w_in, w_out, top)
        mlp_held = mlp_grads(plan.after(g_top[0]), parts, dy_two, top, n_layers, None)
        d_one = own(dy_one) + rms_pull(own(y_one), later(g_back, mlp_held[0]).astype(F32))
        g_sum, x_two_out = scatter(g_top), own(y_two)
        d_two, attn_held, last = own(dy_two), None, mlp_held[0]

        for layer_pair in reversed(range(n_pairs)):
            s_one, s_two = saved_one[layer_pair], saved_two[layer_pair]
            mid, low = 2 * layer_pair + 1, 2 * layer_pair
            g_part = mlp_forward(plan.after(last), s_one, w_in, w_out, low)
            d_one_bf = gather(d_one.astype(BF16), g_part[0])
            mid_back, attn_held, _ = attn_back(
                plan.after(g_part[0]), s_two, d_one_bf, w_t, w_o2, mid, n_heads, n_layers, attn_held
            )
            x_two_shard = x_two_out - later(g_sum, mid_back[0])
            f_in = gather(rms_bf(x_two_shard))
            g_sum, x_two_out = scatter(g_part), own(s_two)
            f_back, attn_held, _ = attn_back(
                plan.after(mid_back[0]), f_in, d_one_bf, w_t, w_o2, mid + 1, n_heads, n_layers, attn_held
            )
            d_two = d_two + rms_pull(x_two_shard, scatter(f_back).astype(F32))
            mid_d = gather(d_two.astype(BF16))
            d_two = d_two + rms_pull(own(s_two), scatter(mid_back).astype(F32))
            low_d = gather(d_two.astype(BF16))
            dx_pair, mid_parts = mlp_back(plan, s_one, mid_d, w_in, w_out, mid)
            x_two_shard = x_two_out - later(g_sum, dx_pair[0])
            dx_pair, low_parts = mlp_back(plan, s_one, low_d, w_in, w_out, low, dx_pair)
            heads, x_two = attn_forward(plan.after(dx_pair[0]), gather(x_two_shard), w_t, low, n_heads)
            d_one = d_one + rms_pull(own(s_one), scatter(dx_pair).astype(F32))
            if layer_pair:
                last = dx_pair[0]
                g_sum, x_two_out = jnp.zeros_like(x_two_shard), x_two_shard
                mlp_held = mlp_grads(plan, mid_parts, mid_d, mid, n_layers, mlp_held)
                mlp_held = mlp_grads(plan, low_parts, low_d, low, n_layers, mlp_held)
        f_back, attn_held, d_one_full = attn_back(
            plan.after(heads), x_two, gather(d_one), w_t, w_o2, 0, n_heads, n_layers, attn_held, True
        )
        heads_all = gather(heads)
        d_two = d_two + rms_pull(x_two_shard, scatter((f_back[0], later(f_back[1], heads_all[1]))).astype(F32))
        tail = plan.after(f_back[0])
        mlp_held = mlp_grads(tail, mid_parts, mid_d, 1, n_layers, mlp_held)
        mlp_held = mlp_grads(tail, low_parts, low_d, 0, n_layers, mlp_held)
        x_one = project_out(tail, s_one, heads_all, wo_low)
        d_two_full = in_order(plan, gather(d_two, x_one, mlp_held[0]))
        d_w = jnp.transpose(attn_held[0].reshape(n_layers, 3, n_heads, size, width), (0, 4, 1, 2, 3))
        d_wo = attn_held[1].reshape(n_layers, n_heads, size, width)
        return (x_one, x_two, d_one_full, d_two_full, d_w, d_wo) + tuple(mlp_held)

    return jax.shard_map(
        per_device,
        mesh=mesh,
        in_specs=(act_spec,) * 4 + (saved_spec,) * 2 + weight_specs,
        out_specs=(act_spec,) * 4 + grad_specs,
        check_vma=False,
    )
```

```python
import functools

import jax
import jax.numpy as jnp
from jax import lax
from jax.experimental import pallas as pl
from jax.experimental.pallas import tpu as pltpu
from jax.sharding import PartitionSpec as P

EPS = 1e-6
F32, BF16 = jnp.float32, jnp.bfloat16
STEP = 2
VMEM = 60 * 1024 * 1024


def dot(lhs, rhs, lhs_dim, rhs_dim):
    return lax.dot_general(lhs, rhs, (((lhs_dim,), (rhs_dim,)), ((), ())), preferred_element_type=F32)


def later(value, *others):
    return lax.optimization_barrier((value,) + others)[0]


def rms_scale(state):
    return lax.rsqrt(jnp.mean(state * state, axis=-1, keepdims=True) + EPS)


def rms_bf(state):
    return (state * rms_scale(state)).astype(BF16)


def rms_pull(state, cot):
    scale = rms_scale(state)
    normed = state * scale
    return scale * (cot - normed * jnp.mean(normed * cot, axis=-1, keepdims=True))


class Plan:
    def __init__(self, gate, n_seq):
        self.gate = gate
        self.n_seq = n_seq

    def after(self, *values):
        return Plan(later(self.gate, *values), self.n_seq)

    @staticmethod
    def seqs(array, slot=None):
        rows, cols = array.shape[-2:]
        if array.ndim == 4:
            return pl.BlockSpec((STEP, None, rows, cols), lambda g, gate: (g, slot, 0, 0))
        return pl.BlockSpec((STEP, rows, cols), lambda g, gate: (g, 0, 0))

    @staticmethod
    def layer(index, rows, cols):
        return pl.BlockSpec((None, rows, cols), lambda g, gate: (index, 0, 0))

    def call(self, body, name, in_specs, out_specs, out_shape, args, flops, aliases=None):
        n_bytes = sum(x.size * x.dtype.itemsize for x in out_shape)
        return pl.pallas_call(
            body,
            name=name,
            grid_spec=pltpu.PrefetchScalarGridSpec(
                num_scalar_prefetch=1, grid=(self.n_seq // STEP,), in_specs=in_specs, out_specs=out_specs
            ),
            out_shape=out_shape,
            input_output_aliases=aliases or {},
            cost_estimate=pl.CostEstimate(flops=int(flops), bytes_accessed=int(n_bytes), transcendentals=0),
            compiler_params=pltpu.CompilerParams(dimension_semantics=("arbitrary",), vmem_limit_bytes=VMEM),
        )(self.gate, *args)


def flat(ref):
    return ref[...].reshape(-1, ref.shape[-1])


def put(ref, value):
    ref[...] = value.astype(ref.dtype).reshape(ref.shape)


def accumulate(pairs):
    @pl.when(pl.program_id(0) == 0)
    def _():
        for ref, value in pairs:
            ref[...] = value

    @pl.when(pl.program_id(0) > 0)
    def _():
        for ref, value in pairs:
            ref[...] += value


def gelu_parts(hidden):
    root = (2.0 / jnp.pi) ** 0.5
    square = hidden * hidden
    bent = jnp.tanh(root * (hidden + 0.044715 * (square * hidden)))
    cdf = 0.5 * (1.0 + bent)
    return hidden * cdf, bent, cdf, root, square


def mlp_forward(plan, state, w_in, w_out, layer):
    n_seq, rows, width = state.shape
    ff = w_in.shape[-1]

    def body(gate, x_ref, win_ref, wout_ref, out_ref):
        act = gelu_parts(dot(rms_bf(flat(x_ref)), win_ref[...], 1, 0))[0].astype(BF16)
        put(out_ref, dot(act, wout_ref[...], 1, 0))

    return plan.call(
        body,
        "mlp_forward",
        [plan.seqs(state), plan.layer(layer, width, ff), plan.layer(layer, ff, width)],
        [plan.seqs(state)],
        [jax.ShapeDtypeStruct(state.shape, F32)],
        (state, w_in, w_out),
        4 * n_seq * rows * width * ff,
    )[0]


def mlp_back(plan, state, d_out, slot, w_in, w_out, layer, extra=None):
    n_seq, rows, width = state.shape
    ff = w_in.shape[-1]
    n_e = 0 if extra is None else 1

    def body(gate, x_ref, d_ref, win_ref, wout_ref, *refs):
        dx_ref, a_ref, act_ref, dh_ref = refs[n_e:]
        normed = rms_bf(flat(x_ref))
        hidden = dot(normed, win_ref[...], 1, 0)
        d_act = dot(flat(d_ref).astype(BF16), wout_ref[...], 1, 1)
        act, bent, cdf, root, square = gelu_parts(hidden)
        slope = cdf + 0.5 * hidden * (1.0 - bent * bent) * (root * (1.0 + 3.0 * 0.044715 * square))
        d_hidden = (slope * d_act).astype(BF16)
        d_x = dot(d_hidden, win_ref[...], 1, 1)
        if n_e:
            d_x = d_x + flat(refs[0]).astype(F32)
        put(dx_ref, d_x)
        put(a_ref, normed)
        put(act_ref, act)
        put(dh_ref, d_hidden)

    in_specs = [plan.seqs(state), plan.seqs(d_out, slot), plan.layer(layer, width, ff), plan.layer(layer, ff, width)]
    args = [state, d_out, w_in, w_out]
    if n_e:
        in_specs.append(plan.seqs(extra))
        args.append(extra)
    wide = jax.ShapeDtypeStruct((n_seq, rows, width), BF16)
    narrow = jax.ShapeDtypeStruct((n_seq, rows, ff), BF16)
    out_shape = [wide, wide, narrow, narrow]
    outs = plan.call(
        body, "mlp_back", in_specs, [plan.seqs(x) for x in out_shape], out_shape, args, 6 * n_seq * rows * width * ff
    )
    return outs[0], tuple(outs[1:])


def mlp_grads(plan, parts, d_out, slot, layer, n_layers, held):
    normed, act, d_hidden = parts
    n_seq, rows, width = normed.shape
    ff = act.shape[-1]
    n_held = 0 if held is None else 2

    def body(gate, a_ref, act_ref, dh_ref, d_ref, *refs):
        dwin_ref, dwout_ref = refs[n_held:]
        d_win = dot(flat(a_ref), flat(dh_ref), 0, 0)
        d_wout = dot(flat(act_ref), flat(d_ref).astype(BF16), 0, 0)
        accumulate([(dwin_ref, d_win), (dwout_ref, d_wout)])

    in_specs = [plan.seqs(normed), plan.seqs(act), plan.seqs(d_hidden), plan.seqs(d_out, slot)]
    args = [normed, act, d_hidden, d_out]
    aliases = {}
    if n_held:
        aliases = {len(args) + 1 + i: i for i in range(n_held)}
        in_specs += [pl.BlockSpec(memory_space=pl.ANY)] * n_held
        args += list(held)
    return plan.call(
        body,
        "mlp_grads",
        in_specs,
        [plan.layer(layer, width, ff), plan.layer(layer, ff, width)],
        [jax.ShapeDtypeStruct((n_layers, width, ff), F32), jax.ShapeDtypeStruct((n_layers, ff, width), F32)],
        args,
        4 * n_seq * rows * width * ff,
        aliases,
    )


def softmax(scores):
    powers = jnp.exp(scores - jnp.max(scores, axis=-1, keepdims=True))
    return powers / jnp.sum(powers, axis=-1, keepdims=True)


def cut(value, row, size, col, rows):
    return value[row * size :][:size][:, col * rows :][:, :rows].astype(BF16)


def attn_forward(plan, state, w_t, layer, n_heads):
    n_seq, rows, width = state.shape
    depth = w_t.shape[1]
    size = depth // 3 // n_heads

    def body(gate, x_ref, w_ref, out_ref, state_ref):
        state_ref[...] = x_ref[...]
        qkv = dot(w_ref[...], rms_bf(flat(x_ref)), 1, 1)
        cols = []
        for col in range(STEP):
            outs = []
            for head in range(n_heads):
                q, k, v = (cut(qkv, kind * n_heads + head, size, col, rows) for kind in range(3))
                probs = softmax(dot(q, k, 0, 0) * size ** -0.5).astype(BF16)
                outs.append(dot(v, probs, 1, 1))
            cols.append(jnp.concatenate(outs, axis=0))
        out_ref[...] = jnp.concatenate(cols, axis=1).astype(BF16)

    return plan.call(
        body,
        "attn_forward",
        [plan.seqs(state), plan.layer(layer, depth, width)],
        [pl.BlockSpec((depth // 3, STEP * rows), lambda g, gate: (0, g)), plan.seqs(state)],
        [jax.ShapeDtypeStruct((depth // 3, n_seq * rows), BF16), jax.ShapeDtypeStruct(state.shape, F32)],
        (state, w_t),
        2 * n_seq * rows * width * depth,
    )


def attn_back(plan, state, d_out, w_t, w_o, layer, n_heads, n_layers, held, keep_d=False):
    n_seq, rows, width = state.shape
    depth = w_t.shape[1]
    size = depth // 3 // n_heads
    n_held = 0 if held is None else 2

    def body(gate, x_ref, d_ref, w_ref, wo_ref, *refs):
        dx_ref, dw_ref, dwo_ref = refs[n_held:][:3]
        normed = flat(x_ref) if x_ref.dtype == BF16 else rms_bf(flat(x_ref))
        d_bf = flat(d_ref).astype(BF16)
        if keep_d:
            refs[-1][...] = d_ref[...]
        qkv = dot(w_ref[...], normed, 1, 1)
        d_heads = dot(wo_ref[...], d_bf, 1, 1)
        out_cols, d_cols = [], []
        for col in range(STEP):
            outs, d_parts = [], [[], [], []]
            for head in range(n_heads):
                q, k, v = (cut(qkv, kind * n_heads + head, size, col, rows) for kind in range(3))
                d_head = cut(d_heads, head, size, col, rows)
                probs = softmax(dot(q, k, 0, 0) * size ** -0.5)
                probs_bf = probs.astype(BF16)
                outs.append(dot(v, probs_bf, 1, 1))
                d_probs = dot(d_head, v, 0, 0)
                d_scores = probs * (d_probs - jnp.sum(d_probs * probs, axis=-1, keepdims=True)) * size ** -0.5
                d_scores = d_scores.astype(BF16)
                d_parts[0].append(dot(k, d_scores, 1, 1))
                d_parts[1].append(dot(q, d_scores, 1, 0))
                d_parts[2].append(dot(d_head, probs_bf, 1, 0))
            out_cols.append(jnp.concatenate(outs, axis=0))
            d_cols.append(jnp.concatenate(d_parts[0] + d_parts[1] + d_parts[2], axis=0))
        d_qkv = jnp.concatenate(d_cols, axis=1).astype(BF16)
        put(dx_ref, dot(d_qkv, w_ref[...], 0, 0))
        heads = jnp.concatenate(out_cols, axis=1).astype(BF16)
        accumulate([(dw_ref, dot(d_qkv, normed, 1, 0)), (dwo_ref, dot(heads, d_bf, 1, 0))])

    in_specs = [plan.seqs(state), plan.seqs(d_out), plan.layer(layer, depth, width), plan.layer(layer, depth // 3, width)]
    args = [state, d_out, w_t, w_o]
    aliases = {}
    if n_held:
        aliases = {len(args) + 1 + i: 1 + i for i in range(n_held)}
        in_specs += [pl.BlockSpec(memory_space=pl.ANY)] * n_held
        args += list(held)
    out_specs = [plan.seqs(state), plan.layer(layer, depth, width), plan.layer(layer, depth // 3, width)]
    out_shape = [
        jax.ShapeDtypeStruct(state.shape, BF16),
        jax.ShapeDtypeStruct((n_layers, depth, width), F32),
        jax.ShapeDtypeStruct((n_layers, depth // 3, width), F32),
    ]
    if keep_d:
        out_specs.append(plan.seqs(d_out))
        out_shape.append(jax.ShapeDtypeStruct(d_out.shape, d_out.dtype))
    outs = plan.call(body, "attn_back", in_specs, out_specs, out_shape, args, 8 * n_seq * rows * width * depth, aliases)
    return outs[0], tuple(outs[1:3]), (outs[3] if keep_d else None)


def project_out(plan, base, heads, w_o):
    n_seq, rows, width = base.shape
    depth = heads.shape[0]

    def body(gate, x_ref, h_ref, w_ref, out_ref):
        put(out_ref, flat(x_ref) - dot(h_ref[...], w_ref[...], 0, 0))

    return plan.call(
        body,
        "project_out",
        [
            plan.seqs(base),
            pl.BlockSpec((depth, STEP * rows), lambda g, gate: (0, g)),
            pl.BlockSpec((depth, width), lambda g, gate: (0, 0)),
        ],
        [plan.seqs(base)],
        [jax.ShapeDtypeStruct(base.shape, F32)],
        (base, heads, w_o),
        2 * n_seq * rows * width * depth,
    )[0]


def solution(mesh):
    act_spec = P("dp", None, None)
    saved_spec = P(None, "dp", None, None)
    weight_specs = (P(None, None, None, "tp", None), P(None, "tp", None, None), P(None, None, "tp"), P(None, "tp", None))
    grad_specs = (P("dp", None, None, "tp", None), P("dp", "tp", None, None), P("dp", None, "tp"), P("dp", "tp", None))

    def scatter(part):
        return lax.psum_scatter(part, "tp", scatter_dimension=0, tiled=True)

    def gather(shard, *others):
        return later(lax.all_gather(shard, "tp", axis=0, tiled=True), *others)

    def per_device(y_one, y_two, dy_one, dy_two, saved_one, saved_two, w_qkv, w_o, w_in, w_out):
        n_layers, width, _, n_heads, size = w_qkv.shape
        n_pairs = saved_one.shape[0]
        me = lax.axis_index("tp")
        plan = Plan(me.reshape(1).astype(jnp.int32), y_one.shape[0])
        w_t = jnp.transpose(w_qkv, (0, 2, 3, 4, 1)).reshape(n_layers, 3 * n_heads * size, width)
        w_o2 = w_o.reshape(n_layers, n_heads * size, width)

        def own(state):
            return lax.dynamic_slice_in_dim(state, me, 1, 0)

        top = n_layers - 1
        dx, parts = mlp_back(plan, y_one, dy_two, None, w_in, w_out, top)
        g_back = scatter(dx)
        g_part = mlp_forward(plan.after(dx), y_one, w_in, w_out, top)
        d_one = own(dy_one) + rms_pull(own(y_one), later(g_back, g_part).astype(F32))
        d_shard = d_one.astype(BF16)
        mlp_held = mlp_grads(plan.after(d_shard), parts, dy_two, None, top, n_layers, None)
        g_sum, x_two_out = scatter(later(g_part, d_shard)), own(y_two)
        d_two, attn_held, last = own(dy_two), None, mlp_held[0]

        for layer_pair in reversed(range(n_pairs)):
            s_one, s_two = saved_one[layer_pair], saved_two[layer_pair]
            mid, low = 2 * layer_pair + 1, 2 * layer_pair
            g_part = mlp_forward(plan.after(last), s_one, w_in, w_out, low)
            d_one_bf = gather(d_shard, g_part)
            mid_back, attn_held, _ = attn_back(plan, s_two, d_one_bf, w_t, w_o2, mid, n_heads, n_layers, attn_held)
            x_two_shard = x_two_out - later(g_sum, mid_back)
            f_shard = rms_bf(x_two_shard)
            f_in = gather(f_shard)
            mid_sum = scatter(later(mid_back, f_shard))
            f_back, attn_held, _ = attn_back(plan, f_in, d_one_bf, w_t, w_o2, mid + 1, n_heads, n_layers, attn_held)
            g_sum, x_two_out = scatter(later(g_part, f_shard)), own(s_two)
            mid_two = d_two + rms_pull(x_two_shard, scatter(f_back).astype(F32))
            d_two = mid_two + rms_pull(own(s_two), later(mid_sum, f_back).astype(F32))
            both_d = gather(jnp.stack([mid_two.astype(BF16), d_two.astype(BF16)], axis=1))
            dx, mid_parts = mlp_back(plan, s_one, both_d, 0, w_in, w_out, mid)
            dx, low_parts = mlp_back(plan, s_one, both_d, 1, w_in, w_out, low, dx)
            x_two_shard = x_two_out - later(g_sum, dx)
            d_one = d_one + rms_pull(own(s_one), scatter(dx).astype(F32))
            heads, x_two = attn_forward(plan, gather(x_two_shard, d_one), w_t, low, n_heads)
            if layer_pair:
                d_shard, last = d_one.astype(BF16), dx
                g_sum, x_two_out = jnp.zeros_like(x_two_shard), x_two_shard
                mlp_held = mlp_grads(plan, mid_parts, both_d, 0, mid, n_layers, mlp_held)
                mlp_held = mlp_grads(plan, low_parts, both_d, 1, low, n_layers, mlp_held)
        f_back, attn_held, d_one_full = attn_back(
            plan.after(heads), x_two, gather(d_one), w_t, w_o2, 0, n_heads, n_layers, attn_held, True
        )
        heads_all, wo_all = gather(heads, f_back), gather(w_o2[0], f_back)
        d_two = d_two + rms_pull(x_two_shard, scatter(later(f_back, heads_all, wo_all)).astype(F32))
        tail = plan.after(f_back)
        mlp_held = mlp_grads(tail, mid_parts, both_d, 0, 1, n_layers, mlp_held)
        mlp_held = mlp_grads(tail, low_parts, both_d, 1, 0, n_layers, mlp_held)
        x_one = project_out(tail, s_one, heads_all, wo_all)
        d_two_full = gather(d_two, x_one, mlp_held[0])
        d_w = jnp.transpose(attn_held[0].reshape(n_layers, 3, n_heads, size, width), (0, 4, 1, 2, 3))
        d_wo = attn_held[1].reshape(n_layers, n_heads, size, width)
        return (x_one, x_two, d_one_full, d_two_full, d_w, d_wo) + tuple(mlp_held)

    return jax.shard_map(
        per_device,
        mesh=mesh,
        in_specs=(act_spec,) * 4 + (saved_spec,) * 2 + weight_specs,
        out_specs=(act_spec,) * 4 + grad_specs,
        check_vma=False,
    )
```

```python
import jax
import jax.numpy as jnp
from jax import lax
from jax.experimental import pallas as pl
from jax.experimental.pallas import tpu as pltpu
from jax.sharding import PartitionSpec as P


EPS = 1e-6
F32, BF16 = jnp.float32, jnp.bfloat16
CORES = 2
STEP = 2
VMEM = 60 * 1024 * 1024


def dot(lhs, rhs, lhs_dim, rhs_dim):
    return lax.dot_general(lhs, rhs, (((lhs_dim,), (rhs_dim,)), ((), ())), preferred_element_type=F32)


def later(value, *others):
    return lax.optimization_barrier((value,) + others)[0]


def rms_scale(state):
    return lax.rsqrt(jnp.mean(state * state, axis=-1, keepdims=True) + EPS)


def rms_bf(state):
    return (state * rms_scale(state)).astype(BF16)


def rms_pull(state, cot):
    scale = rms_scale(state)
    normed = state * scale
    return scale * (cot - normed * jnp.mean(normed * cot, axis=-1, keepdims=True))


class Plan:
    def __init__(self, gate, n_seq):
        self.gate = gate
        self.n_seq = n_seq

    def after(self, *values):
        return Plan(later(self.gate, *values), self.n_seq)

    @staticmethod
    def seqs(array, slot=None):
        rows, cols = array.shape[-2:]
        if array.ndim == 4:
            return pl.BlockSpec((STEP, None, rows, cols), lambda g, gate: (g, slot, 0, 0))
        return pl.BlockSpec((STEP, rows, cols), lambda g, gate: (g, 0, 0))

    @staticmethod
    def layer(index, rows, cols):
        return pl.BlockSpec((None, rows, cols), lambda g, gate: (index, 0, 0))

    def call(self, body, in_specs, out_specs, out_shape, args, flops, aliases=None):
        n_bytes = sum(x.size * x.dtype.itemsize for x in out_shape)
        return pl.pallas_call(
            body,
            grid_spec=pltpu.PrefetchScalarGridSpec(
                num_scalar_prefetch=1, grid=(self.n_seq // STEP,), in_specs=in_specs, out_specs=out_specs
            ),
            out_shape=out_shape,
            input_output_aliases=aliases or {},
            cost_estimate=pl.CostEstimate(flops=int(flops), bytes_accessed=int(n_bytes), transcendentals=0),
            compiler_params=pltpu.CompilerParams(dimension_semantics=("arbitrary",), vmem_limit_bytes=VMEM),
        )(self.gate, *args)


def flat(ref):
    return ref[...].reshape(-1, ref.shape[-1])


def put(ref, value):
    ref[...] = value.astype(ref.dtype).reshape(ref.shape)


def accumulate(pairs):
    @pl.when(pl.program_id(0) == 0)
    def _():
        for ref, value in pairs:
            ref[...] = value

    @pl.when(pl.program_id(0) > 0)
    def _():
        for ref, value in pairs:
            ref[...] += value


def gelu_parts(hidden):
    root = (2.0 / jnp.pi) ** 0.5
    square = hidden * hidden
    bent = jnp.tanh(root * (hidden + 0.044715 * (square * hidden)))
    cdf = 0.5 * (1.0 + bent)
    return hidden * cdf, bent, cdf, root, square


def mlp_forward(plan, state, w_in, w_out, layer):
    n_seq, rows, width = state.shape
    ff = w_in.shape[-1]

    def body(gate, x_ref, win_ref, wout_ref, out_ref):
        act = gelu_parts(dot(rms_bf(flat(x_ref)), win_ref[...], 1, 0))[0].astype(BF16)
        put(out_ref, dot(act, wout_ref[...], 1, 0))

    return plan.call(
        body,
        [plan.seqs(state), plan.layer(layer, width, ff), plan.layer(layer, ff, width)],
        [plan.seqs(state)],
        [jax.ShapeDtypeStruct(state.shape, F32)],
        (state, w_in, w_out),
        4 * n_seq * rows * width * ff,
    )[0]


def mlp_back(plan, state, d_out, slot, w_in, w_out, layer, extra=None):
    n_seq, rows, width = state.shape
    ff = w_in.shape[-1]
    n_e = 0 if extra is None else 1

    def body(gate, x_ref, d_ref, win_ref, wout_ref, *refs):
        dx_ref, a_ref, act_ref, dh_ref = refs[n_e:]
        normed = rms_bf(flat(x_ref))
        hidden = dot(normed, win_ref[...], 1, 0)
        d_act = dot(flat(d_ref).astype(BF16), wout_ref[...], 1, 1)
        act, bent, cdf, root, square = gelu_parts(hidden)
        slope = cdf + 0.5 * hidden * (1.0 - bent * bent) * (root * (1.0 + 3.0 * 0.044715 * square))
        d_hidden = (slope * d_act).astype(BF16)
        d_x = dot(d_hidden, win_ref[...], 1, 1)
        if n_e:
            d_x = d_x + flat(refs[0]).astype(F32)
        put(dx_ref, d_x)
        put(a_ref, normed)
        put(act_ref, act)
        put(dh_ref, d_hidden)

    in_specs = [plan.seqs(state), plan.seqs(d_out, slot), plan.layer(layer, width, ff), plan.layer(layer, ff, width)]
    args = [state, d_out, w_in, w_out]
    if n_e:
        in_specs.append(plan.seqs(extra))
        args.append(extra)
    wide = jax.ShapeDtypeStruct((n_seq, rows, width), BF16)
    narrow = jax.ShapeDtypeStruct((n_seq, rows, ff), BF16)
    out_shape = [wide, wide, narrow, narrow]
    outs = plan.call(body, in_specs, [plan.seqs(x) for x in out_shape], out_shape, args, 6 * n_seq * rows * width * ff)
    return outs[0], tuple(outs[1:])


def mlp_grads(plan, parts, d_out, slot, layer, n_layers, held):
    normed, act, d_hidden = parts
    n_seq, rows, width = normed.shape
    ff = act.shape[-1]
    n_held = 0 if held is None else 2

    def body(gate, a_ref, act_ref, dh_ref, d_ref, *refs):
        dwin_ref, dwout_ref = refs[n_held:]
        d_win = dot(flat(a_ref), flat(dh_ref), 0, 0)
        d_wout = dot(flat(act_ref), flat(d_ref).astype(BF16), 0, 0)
        accumulate([(dwin_ref, d_win), (dwout_ref, d_wout)])

    in_specs = [plan.seqs(normed), plan.seqs(act), plan.seqs(d_hidden), plan.seqs(d_out, slot)]
    args = [normed, act, d_hidden, d_out]
    aliases = {}
    if n_held:
        aliases = {len(args) + 1 + i: i for i in range(n_held)}
        in_specs += [pl.BlockSpec(memory_space=pl.ANY)] * n_held
        args += list(held)
    return plan.call(
        body,
        in_specs,
        [plan.layer(layer, width, ff), plan.layer(layer, ff, width)],
        [jax.ShapeDtypeStruct((n_layers, width, ff), F32), jax.ShapeDtypeStruct((n_layers, ff, width), F32)],
        args,
        4 * n_seq * rows * width * ff,
        aliases,
    )


def softmax(scores):
    powers = jnp.exp(scores - jnp.max(scores, axis=-1, keepdims=True))
    return powers / jnp.sum(powers, axis=-1, keepdims=True)


def cut(value, row, size, col, rows):
    return value[row * size :][:size][:, col * rows :][:, :rows].astype(BF16)


def attn_forward(plan, state, w_t, layer, n_heads):
    n_seq, rows, width = state.shape
    depth = w_t.shape[1]
    size = depth // 3 // n_heads

    def body(gate, x_ref, w_ref, out_ref, state_ref):
        state_ref[...] = x_ref[...]
        qkv = dot(w_ref[...], rms_bf(flat(x_ref)), 1, 1)
        cols = []
        for col in range(STEP):
            outs = []
            for head in range(n_heads):
                q, k, v = (cut(qkv, kind * n_heads + head, size, col, rows) for kind in range(3))
                probs = softmax(dot(q, k, 0, 0) * size ** -0.5).astype(BF16)
                outs.append(dot(v, probs, 1, 1))
            cols.append(jnp.concatenate(outs, axis=0))
        out_ref[...] = jnp.concatenate(cols, axis=1).astype(BF16)

    return plan.call(
        body,
        [plan.seqs(state), plan.layer(layer, depth, width)],
        [pl.BlockSpec((depth // 3, STEP * rows), lambda g, gate: (0, g)), plan.seqs(state)],
        [jax.ShapeDtypeStruct((depth // 3, n_seq * rows), BF16), jax.ShapeDtypeStruct(state.shape, F32)],
        (state, w_t),
        2 * n_seq * rows * width * depth,
    )


def attn_back(plan, state, d_out, w_t, w_o, layer, n_heads, n_layers, held, keep_d=False):
    n_seq, rows, width = state.shape
    depth = w_t.shape[1]
    size = depth // 3 // n_heads
    n_held = 0 if held is None else 2

    def body(gate, x_ref, d_ref, w_ref, wo_ref, *refs):
        dx_ref, dw_ref, dwo_ref = refs[n_held:][:3]
        normed = flat(x_ref) if x_ref.dtype == BF16 else rms_bf(flat(x_ref))
        d_bf = flat(d_ref).astype(BF16)
        if keep_d:
            refs[-1][...] = d_ref[...]
        qkv = dot(w_ref[...], normed, 1, 1)
        d_heads = dot(wo_ref[...], d_bf, 1, 1)
        out_cols, d_cols = [], []
        for col in range(STEP):
            outs, d_parts = [], [[], [], []]
            for head in range(n_heads):
                q, k, v = (cut(qkv, kind * n_heads + head, size, col, rows) for kind in range(3))
                d_head = cut(d_heads, head, size, col, rows)
                probs = softmax(dot(q, k, 0, 0) * size ** -0.5)
                probs_bf = probs.astype(BF16)
                outs.append(dot(v, probs_bf, 1, 1))
                d_probs = dot(d_head, v, 0, 0)
                d_scores = probs * (d_probs - jnp.sum(d_probs * probs, axis=-1, keepdims=True)) * size ** -0.5
                d_scores = d_scores.astype(BF16)
                d_parts[0].append(dot(k, d_scores, 1, 1))
                d_parts[1].append(dot(q, d_scores, 1, 0))
                d_parts[2].append(dot(d_head, probs_bf, 1, 0))
            out_cols.append(jnp.concatenate(outs, axis=0))
            d_cols.append(jnp.concatenate(d_parts[0] + d_parts[1] + d_parts[2], axis=0))
        d_qkv = jnp.concatenate(d_cols, axis=1).astype(BF16)
        put(dx_ref, dot(d_qkv, w_ref[...], 0, 0))
        heads = jnp.concatenate(out_cols, axis=1).astype(BF16)
        accumulate([(dw_ref, dot(d_qkv, normed, 1, 0)), (dwo_ref, dot(heads, d_bf, 1, 0))])

    in_specs = [plan.seqs(state), plan.seqs(d_out), plan.layer(layer, depth, width), plan.layer(layer, depth // 3, width)]
    args = [state, d_out, w_t, w_o]
    aliases = {}
    if n_held:
        aliases = {len(args) + 1 + i: 1 + i for i in range(n_held)}
        in_specs += [pl.BlockSpec(memory_space=pl.ANY)] * n_held
        args += list(held)
    out_specs = [plan.seqs(state), plan.layer(layer, depth, width), plan.layer(layer, depth // 3, width)]
    out_shape = [
        jax.ShapeDtypeStruct(state.shape, BF16),
        jax.ShapeDtypeStruct((n_layers, depth, width), F32),
        jax.ShapeDtypeStruct((n_layers, depth // 3, width), F32),
    ]
    if keep_d:
        out_specs.append(plan.seqs(d_out))
        out_shape.append(jax.ShapeDtypeStruct(d_out.shape, d_out.dtype))
    outs = plan.call(body, in_specs, out_specs, out_shape, args, 8 * n_seq * rows * width * depth, aliases)
    return outs[0], tuple(outs[1:3]), (outs[3] if keep_d else None)


def project_out(plan, base, heads, w_o):
    n_seq, rows, width = base.shape
    depth = heads.shape[0]

    def body(gate, x_ref, h_ref, w_ref, out_ref):
        put(out_ref, flat(x_ref) - dot(h_ref[...], w_ref[...], 0, 0))

    return plan.call(
        body,
        [
            plan.seqs(base),
            pl.BlockSpec((depth, STEP * rows), lambda g, gate: (0, g)),
            pl.BlockSpec((depth, width), lambda g, gate: (0, 0)),
        ],
        [plan.seqs(base)],
        [jax.ShapeDtypeStruct(base.shape, F32)],
        (base, heads, w_o),
        2 * n_seq * rows * width * depth,
    )[0]


def solution(mesh):
    act_spec = P("dp", None, None)
    saved_spec = P(None, "dp", None, None)
    weight_specs = (P(None, None, None, "tp", None), P(None, "tp", None, None), P(None, None, "tp"), P(None, "tp", None))
    grad_specs = (P("dp", None, None, "tp", None), P("dp", "tp", None, None), P("dp", None, "tp"), P("dp", "tp", None))

    def scatter(part):
        return lax.psum_scatter(part, "tp", scatter_dimension=0, tiled=True)

    def gather(shard, *others):
        return later(lax.all_gather(shard, "tp", axis=0, tiled=True), *others)

    n_tp = mesh.shape["tp"]
    chips = n_tp // CORES

    def shift(value, hops):
        pairs = [(i, (i // CORES + hops) % chips * CORES + i % CORES) for i in range(n_tp)]
        return lax.ppermute(value, "tp", pairs)

    def swap(value):
        return lax.ppermute(value, "tp", [(i, i + 1 - 2 * (i % CORES)) for i in range(n_tp)])

    def ring_scatter(part):
        chip, core = lax.div(lax.axis_index("tp"), CORES), lax.rem(lax.axis_index("tp"), CORES)
        split = part.reshape((chips, CORES) + part.shape[1:])
        half = part.shape[1] // 2
        far = swap(lax.dynamic_index_in_dim(split, 1 - core, 1, False))
        mine = lax.dynamic_index_in_dim(split, core, 1, False) + far
        ahead, across, behind, here = (
            lax.dynamic_index_in_dim(mine, lax.rem(chip + hops, chips), 0, False) for hops in (1, 2, 3, 0)
        )
        from_back, from_front = shift(across[:half], 1), shift(across[half:], -1)
        back_low, front_high = shift(ahead[half:], 1), shift(behind[:half], -1)

        def finish(second, third):
            back_high = shift(ahead[:half] + later(from_back, *second), 1)
            front_low = shift(behind[half:] + later(from_front, *second), -1)
            high = later(back_high, *third) + front_high
            low = later(front_low, *third) + back_low
            return (here + jnp.concatenate([high, low], axis=0))[None]

        return finish, mine

    def ring_gather(shard, second, third):
        chip, core = lax.div(lax.axis_index("tp"), CORES), lax.rem(lax.axis_index("tp"), CORES)
        rows = shard.shape[0]
        half = rows // 2
        back, front = shift(shard, 1), shift(shard, -1)
        back, front = later(back, *second), later(front, *second)
        far_low, far_high = shift(back[:half], 1), shift(front[half:], -1)
        across = jnp.concatenate([later(far_low, *third), later(far_high, *third)], axis=0)
        whole = jnp.zeros((n_tp,) + shard.shape, shard.dtype)
        for hops, piece in ((0, shard), (chips - 1, back), (1, front), (2, across)):
            place = lax.rem(chip + hops, chips) * CORES
            other = later(swap(piece), *third)
            whole = lax.dynamic_update_slice_in_dim(whole, later(piece, *third)[None], place + core, 0)
            whole = lax.dynamic_update_slice_in_dim(whole, other[None], place + 1 - core, 0)
        return whole

    def per_device(y_one, y_two, dy_one, dy_two, saved_one, saved_two, w_qkv, w_o, w_in, w_out):
        n_layers, width, _, n_heads, size = w_qkv.shape
        n_pairs = saved_one.shape[0]
        me = lax.axis_index("tp")
        plan = Plan(me.reshape(1).astype(jnp.int32), y_one.shape[0])
        w_t = jnp.transpose(w_qkv, (0, 2, 3, 4, 1)).reshape(n_layers, 3 * n_heads * size, width)
        w_o2 = w_o.reshape(n_layers, n_heads * size, width)

        def own(state):
            return lax.dynamic_slice_in_dim(state, me, 1, 0)

        top = n_layers - 1
        dx, parts = mlp_back(plan, y_one, dy_two, None, w_in, w_out, top)
        g_back = scatter(dx)
        g_part = mlp_forward(plan.after(dx), y_one, w_in, w_out, top)
        d_one = own(dy_one) + rms_pull(own(y_one), later(g_back, g_part).astype(F32))
        d_shard = d_one.astype(BF16)
        mlp_held = mlp_grads(plan.after(d_shard), parts, dy_two, None, top, n_layers, None)
        g_sum, x_two_out = scatter(later(g_part, d_shard)), own(y_two)
        wo_all = ring_gather(w_o2[0], (dx,), (g_part,)).reshape(-1, width)
        d_two, attn_held, last = own(dy_two), None, mlp_held[0]

        for layer_pair in reversed(range(n_pairs)):
            s_one, s_two = saved_one[layer_pair], saved_two[layer_pair]
            mid, low = 2 * layer_pair + 1, 2 * layer_pair
            g_part = mlp_forward(plan.after(last), s_one, w_in, w_out, low)
            d_one_bf = gather(d_shard, g_part)
            finish, chip_sums = ring_scatter(g_part)
            mid_back, attn_held, _ = attn_back(
                plan.after(chip_sums), s_two, d_one_bf, w_t, w_o2, mid, n_heads, n_layers, attn_held
            )
            x_two_shard = x_two_out - later(g_sum, mid_back)
            f_shard = rms_bf(x_two_shard)
            f_in = gather(f_shard)
            mid_sum = scatter(later(mid_back, f_shard))
            f_back, attn_held, _ = attn_back(
                plan, f_in, d_one_bf, w_t, w_o2, mid + 1, n_heads, n_layers, attn_held
            )
            low_two = own(s_two) - finish((f_in,), (f_back,))
            mid_two = d_two + rms_pull(x_two_shard, scatter(f_back).astype(F32))
            d_two = mid_two + rms_pull(own(s_two), later(mid_sum, f_back).astype(F32))
            both_d = gather(jnp.stack([mid_two.astype(BF16), d_two.astype(BF16)], axis=1))
            dx, mid_parts = mlp_back(plan.after(low_two), s_one, both_d, 0, w_in, w_out, mid)
            mid_dx = dx
            dx, low_parts = mlp_back(plan, s_one, both_d, 1, w_in, w_out, low, dx)
            x_two = ring_gather(low_two[0], (mid_dx,), (dx,))
            heads, x_two = attn_forward(plan, x_two, w_t, low, n_heads)
            x_two_shard = low_two
            d_one = d_one + rms_pull(own(s_one), later(scatter(dx), heads).astype(F32))
            if layer_pair:
                d_shard, last = d_one.astype(BF16), dx
                g_sum, x_two_out = jnp.zeros_like(x_two_shard), x_two_shard
                mlp_held = mlp_grads(plan, mid_parts, both_d, 0, mid, n_layers, mlp_held)
                mlp_held = mlp_grads(plan, low_parts, both_d, 1, low, n_layers, mlp_held)
        f_back, attn_held, d_one_full = attn_back(
            plan, x_two, gather(d_one), w_t, w_o2, 0, n_heads, n_layers, attn_held, True
        )
        heads_all = gather(later(heads, d_one), f_back)
        d_two = d_two + rms_pull(x_two_shard, scatter(later(f_back, heads_all)).astype(F32))
        tail = plan.after(f_back)
        mlp_held = mlp_grads(tail, mid_parts, both_d, 0, 1, n_layers, mlp_held)
        mlp_held = mlp_grads(tail, low_parts, both_d, 1, 0, n_layers, mlp_held)
        x_one = project_out(tail, s_one, heads_all, wo_all)
        d_two_full = gather(d_two, x_one, mlp_held[0])
        d_w = jnp.transpose(attn_held[0].reshape(n_layers, 3, n_heads, size, width), (0, 4, 1, 2, 3))
        d_wo = attn_held[1].reshape(n_layers, n_heads, size, width)
        return (x_one, x_two, d_one_full, d_two_full, d_w, d_wo) + tuple(mlp_held)

    return jax.shard_map(
        per_device,
        mesh=mesh,
        in_specs=(act_spec,) * 4 + (saved_spec,) * 2 + weight_specs,
        out_specs=(act_spec,) * 4 + grad_specs,
        check_vma=False,
    )
```

```python
import jax
import jax.numpy as jnp
from jax import lax
from jax.experimental import pallas as pl
from jax.experimental.pallas import tpu as pltpu
from jax.sharding import PartitionSpec as P


EPS = 1e-6
F32, BF16 = jnp.float32, jnp.bfloat16
CORES = 2
STEP = 2
VMEM = 60 * 1024 * 1024


def dot(lhs, rhs, lhs_dim, rhs_dim):
    return lax.dot_general(lhs, rhs, (((lhs_dim,), (rhs_dim,)), ((), ())), preferred_element_type=F32)


def later(value, *others):
    return lax.optimization_barrier((value,) + others)[0]


def rms_scale(state):
    return lax.rsqrt(jnp.mean(state * state, axis=-1, keepdims=True) + EPS)


def rms_bf(state):
    return (state * rms_scale(state)).astype(BF16)


def rms_pull(state, cot):
    scale = rms_scale(state)
    normed = state * scale
    return scale * (cot - normed * jnp.mean(normed * cot, axis=-1, keepdims=True))


class Plan:
    def __init__(self, gate, n_seq):
        self.gate = gate
        self.n_seq = n_seq

    def after(self, *values):
        return Plan(later(self.gate, *values), self.n_seq)

    @staticmethod
    def seqs(array, slot=None):
        rows, cols = array.shape[-2:]
        if array.ndim == 4:
            return pl.BlockSpec((STEP, None, rows, cols), lambda g, gate: (g, slot, 0, 0))
        return pl.BlockSpec((STEP, rows, cols), lambda g, gate: (g, 0, 0))

    @staticmethod
    def layer(index, rows, cols):
        return pl.BlockSpec((None, rows, cols), lambda g, gate: (index, 0, 0))

    def call(self, body, in_specs, out_specs, out_shape, args, flops, aliases=None):
        n_bytes = sum(x.size * x.dtype.itemsize for x in out_shape)
        return pl.pallas_call(
            body,
            grid_spec=pltpu.PrefetchScalarGridSpec(
                num_scalar_prefetch=1, grid=(self.n_seq // STEP,), in_specs=in_specs, out_specs=out_specs
            ),
            out_shape=out_shape,
            input_output_aliases=aliases or {},
            cost_estimate=pl.CostEstimate(flops=int(flops), bytes_accessed=int(n_bytes), transcendentals=0),
            compiler_params=pltpu.CompilerParams(dimension_semantics=("arbitrary",), vmem_limit_bytes=VMEM),
        )(self.gate, *args)


def flat(ref):
    return ref[...].reshape(-1, ref.shape[-1])


def put(ref, value):
    ref[...] = value.astype(ref.dtype).reshape(ref.shape)


def accumulate(pairs):
    @pl.when(pl.program_id(0) == 0)
    def _():
        for ref, value in pairs:
            ref[...] = value

    @pl.when(pl.program_id(0) > 0)
    def _():
        for ref, value in pairs:
            ref[...] += value


def gelu_parts(hidden):
    root = (2.0 / jnp.pi) ** 0.5
    square = hidden * hidden
    bent = jnp.tanh(root * (hidden + 0.044715 * (square * hidden)))
    cdf = 0.5 * (1.0 + bent)
    return hidden * cdf, bent, cdf, root, square


def mlp_forward(plan, state, w_in, w_out, layer):
    n_seq, rows, width = state.shape
    ff = w_in.shape[-1]

    def body(gate, x_ref, win_ref, wout_ref, out_ref):
        act = gelu_parts(dot(rms_bf(flat(x_ref)), win_ref[...], 1, 0))[0].astype(BF16)
        put(out_ref, dot(act, wout_ref[...], 1, 0))

    return plan.call(
        body,
        [plan.seqs(state), plan.layer(layer, width, ff), plan.layer(layer, ff, width)],
        [plan.seqs(state)],
        [jax.ShapeDtypeStruct(state.shape, F32)],
        (state, w_in, w_out),
        4 * n_seq * rows * width * ff,
    )[0]


def mlp_back(plan, state, d_out, slot, w_in, w_out, layer, extra=None):
    n_seq, rows, width = state.shape
    ff = w_in.shape[-1]
    n_e = 0 if extra is None else 1

    def body(gate, x_ref, d_ref, win_ref, wout_ref, *refs):
        dx_ref, a_ref, act_ref, dh_ref = refs[n_e:]
        normed = rms_bf(flat(x_ref))
        hidden = dot(normed, win_ref[...], 1, 0)
        d_act = dot(flat(d_ref).astype(BF16), wout_ref[...], 1, 1)
        act, bent, cdf, root, square = gelu_parts(hidden)
        slope = cdf + 0.5 * hidden * (1.0 - bent * bent) * (root * (1.0 + 3.0 * 0.044715 * square))
        d_hidden = (slope * d_act).astype(BF16)
        d_x = dot(d_hidden, win_ref[...], 1, 1)
        if n_e:
            d_x = d_x + flat(refs[0]).astype(F32)
        put(dx_ref, d_x)
        put(a_ref, normed)
        put(act_ref, act)
        put(dh_ref, d_hidden)

    in_specs = [plan.seqs(state), plan.seqs(d_out, slot), plan.layer(layer, width, ff), plan.layer(layer, ff, width)]
    args = [state, d_out, w_in, w_out]
    if n_e:
        in_specs.append(plan.seqs(extra))
        args.append(extra)
    wide = jax.ShapeDtypeStruct((n_seq, rows, width), BF16)
    narrow = jax.ShapeDtypeStruct((n_seq, rows, ff), BF16)
    out_shape = [wide, wide, narrow, narrow]
    outs = plan.call(body, in_specs, [plan.seqs(x) for x in out_shape], out_shape, args, 6 * n_seq * rows * width * ff)
    return outs[0], tuple(outs[1:])


def mlp_grads(plan, parts, d_out, slot, layer, n_layers, held):
    normed, act, d_hidden = parts
    n_seq, rows, width = normed.shape
    ff = act.shape[-1]
    n_held = 0 if held is None else 2

    def body(gate, a_ref, act_ref, dh_ref, d_ref, *refs):
        dwin_ref, dwout_ref = refs[n_held:]
        d_win = dot(flat(a_ref), flat(dh_ref), 0, 0)
        d_wout = dot(flat(act_ref), flat(d_ref).astype(BF16), 0, 0)
        accumulate([(dwin_ref, d_win), (dwout_ref, d_wout)])

    in_specs = [plan.seqs(normed), plan.seqs(act), plan.seqs(d_hidden), plan.seqs(d_out, slot)]
    args = [normed, act, d_hidden, d_out]
    aliases = {}
    if n_held:
        aliases = {len(args) + 1 + i: i for i in range(n_held)}
        in_specs += [pl.BlockSpec(memory_space=pl.ANY)] * n_held
        args += list(held)
    return plan.call(
        body,
        in_specs,
        [plan.layer(layer, width, ff), plan.layer(layer, ff, width)],
        [jax.ShapeDtypeStruct((n_layers, width, ff), F32), jax.ShapeDtypeStruct((n_layers, ff, width), F32)],
        args,
        4 * n_seq * rows * width * ff,
        aliases,
    )


def softmax(scores):
    powers = jnp.exp(scores - jnp.max(scores, axis=-1, keepdims=True))
    return powers / jnp.sum(powers, axis=-1, keepdims=True)


def cut(value, row, size, col, rows):
    return value[row * size :][:size][:, col * rows :][:, :rows].astype(BF16)


def attn_forward(plan, state, w_t, layer, n_heads):
    n_seq, rows, width = state.shape
    depth = w_t.shape[1]
    size = depth // 3 // n_heads

    def body(gate, x_ref, w_ref, out_ref, state_ref):
        state_ref[...] = x_ref[...]
        qkv = dot(w_ref[...], rms_bf(flat(x_ref)), 1, 1)
        cols = []
        for col in range(STEP):
            outs = []
            for head in range(n_heads):
                q, k, v = (cut(qkv, kind * n_heads + head, size, col, rows) for kind in range(3))
                probs = softmax(dot(q, k, 0, 0) * size ** -0.5).astype(BF16)
                outs.append(dot(v, probs, 1, 1))
            cols.append(jnp.concatenate(outs, axis=0))
        out_ref[...] = jnp.concatenate(cols, axis=1).astype(BF16)

    return plan.call(
        body,
        [plan.seqs(state), plan.layer(layer, depth, width)],
        [pl.BlockSpec((depth // 3, STEP * rows), lambda g, gate: (0, g)), plan.seqs(state)],
        [jax.ShapeDtypeStruct((depth // 3, n_seq * rows), BF16), jax.ShapeDtypeStruct(state.shape, F32)],
        (state, w_t),
        2 * n_seq * rows * width * depth,
    )


def attn_back(plan, state, d_out, w_t, w_o, layer, n_heads, n_layers, held, keep_d=False):
    n_seq, rows, width = state.shape
    depth = w_t.shape[1]
    size = depth // 3 // n_heads
    n_held = 0 if held is None else 2

    def body(gate, x_ref, d_ref, w_ref, wo_ref, *refs):
        dx_ref, dw_ref, dwo_ref = refs[n_held:][:3]
        normed = flat(x_ref) if x_ref.dtype == BF16 else rms_bf(flat(x_ref))
        d_bf = flat(d_ref).astype(BF16)
        if keep_d:
            refs[-1][...] = d_ref[...]
        qkv = dot(w_ref[...], normed, 1, 1)
        d_heads = dot(wo_ref[...], d_bf, 1, 1)
        out_cols, d_cols = [], []
        for col in range(STEP):
            outs, d_parts = [], [[], [], []]
            for head in range(n_heads):
                q, k, v = (cut(qkv, kind * n_heads + head, size, col, rows) for kind in range(3))
                d_head = cut(d_heads, head, size, col, rows)
                probs = softmax(dot(q, k, 0, 0) * size ** -0.5)
                probs_bf = probs.astype(BF16)
                outs.append(dot(v, probs_bf, 1, 1))
                d_probs = dot(d_head, v, 0, 0)
                d_scores = probs * (d_probs - jnp.sum(d_probs * probs, axis=-1, keepdims=True)) * size ** -0.5
                d_scores = d_scores.astype(BF16)
                d_parts[0].append(dot(k, d_scores, 1, 1))
                d_parts[1].append(dot(q, d_scores, 1, 0))
                d_parts[2].append(dot(d_head, probs_bf, 1, 0))
            out_cols.append(jnp.concatenate(outs, axis=0))
            d_cols.append(jnp.concatenate(d_parts[0] + d_parts[1] + d_parts[2], axis=0))
        d_qkv = jnp.concatenate(d_cols, axis=1).astype(BF16)
        put(dx_ref, dot(d_qkv, w_ref[...], 0, 0))
        heads = jnp.concatenate(out_cols, axis=1).astype(BF16)
        accumulate([(dw_ref, dot(d_qkv, normed, 1, 0)), (dwo_ref, dot(heads, d_bf, 1, 0))])

    in_specs = [plan.seqs(state), plan.seqs(d_out), plan.layer(layer, depth, width), plan.layer(layer, depth // 3, width)]
    args = [state, d_out, w_t, w_o]
    aliases = {}
    if n_held:
        aliases = {len(args) + 1 + i: 1 + i for i in range(n_held)}
        in_specs += [pl.BlockSpec(memory_space=pl.ANY)] * n_held
        args += list(held)
    out_specs = [plan.seqs(state), plan.layer(layer, depth, width), plan.layer(layer, depth // 3, width)]
    out_shape = [
        jax.ShapeDtypeStruct(state.shape, BF16),
        jax.ShapeDtypeStruct((n_layers, depth, width), F32),
        jax.ShapeDtypeStruct((n_layers, depth // 3, width), F32),
    ]
    if keep_d:
        out_specs.append(plan.seqs(d_out))
        out_shape.append(jax.ShapeDtypeStruct(d_out.shape, d_out.dtype))
    outs = plan.call(body, in_specs, out_specs, out_shape, args, 8 * n_seq * rows * width * depth, aliases)
    return outs[0], tuple(outs[1:3]), (outs[3] if keep_d else None)


def project_out(plan, base, heads, w_o):
    n_seq, rows, width = base.shape
    depth = heads.shape[0]

    def body(gate, x_ref, h_ref, w_ref, out_ref):
        put(out_ref, flat(x_ref) - dot(h_ref[...], w_ref[...], 0, 0))

    return plan.call(
        body,
        [
            plan.seqs(base),
            pl.BlockSpec((depth, STEP * rows), lambda g, gate: (0, g)),
            pl.BlockSpec((depth, width), lambda g, gate: (0, 0)),
        ],
        [plan.seqs(base)],
        [jax.ShapeDtypeStruct(base.shape, F32)],
        (base, heads, w_o),
        2 * n_seq * rows * width * depth,
    )[0]


def solution(mesh):
    act_spec = P("dp", None, None)
    saved_spec = P(None, "dp", None, None)
    weight_specs = (P(None, None, None, "tp", None), P(None, "tp", None, None), P(None, None, "tp"), P(None, "tp", None))
    grad_specs = (P("dp", None, None, "tp", None), P("dp", "tp", None, None), P("dp", None, "tp"), P("dp", "tp", None))

    def scatter(part):
        return lax.psum_scatter(part, "tp", scatter_dimension=0, tiled=True)

    def gather(shard, *others):
        return later(lax.all_gather(shard, "tp", axis=0, tiled=True), *others)

    n_tp = mesh.shape["tp"]
    chips = n_tp // CORES

    def shift(value, hops):
        pairs = [(i, (i // CORES + hops) % chips * CORES + i % CORES) for i in range(n_tp)]
        return lax.ppermute(value, "tp", pairs)

    def swap(value):
        return lax.ppermute(value, "tp", [(i, i + 1 - 2 * (i % CORES)) for i in range(n_tp)])

    def core_sums(part):
        core = lax.rem(lax.axis_index("tp"), CORES)
        split = part.reshape((chips, CORES) + part.shape[1:])
        far = swap(lax.dynamic_index_in_dim(split, 1 - core, 1, False))
        return (lax.dynamic_index_in_dim(split, core, 1, False).astype(F32) + far.astype(F32)).astype(part.dtype)

    def like_scatter(sums):
        alike = [list(range(core, n_tp, CORES)) for core in range(CORES)]
        return lax.psum_scatter(sums, "tp", scatter_dimension=0, axis_index_groups=alike, tiled=True)

    def ring_scatter(part):
        chip = lax.div(lax.axis_index("tp"), CORES)
        half = part.shape[1] // 2
        mine = core_sums(part)
        ahead, across, behind, here = (
            lax.dynamic_index_in_dim(mine, lax.rem(chip + hops, chips), 0, False) for hops in (1, 2, 3, 0)
        )
        from_back, from_front = shift(across[:half], 1), shift(across[half:], -1)
        back_low, front_high = shift(ahead[half:], 1), shift(behind[:half], -1)

        def finish(second, third):
            back_high = shift(ahead[:half] + later(from_back, *second), 1)
            front_low = shift(behind[half:] + later(from_front, *second), -1)
            high = later(back_high, *third) + front_high
            low = later(front_low, *third) + back_low
            return (here + jnp.concatenate([high, low], axis=0))[None]

        return finish, mine

    def ring_gather(shard, second, third):
        chip, core = lax.div(lax.axis_index("tp"), CORES), lax.rem(lax.axis_index("tp"), CORES)
        rows = shard.shape[0]
        half = rows // 2
        back, front = shift(shard, 1), shift(shard, -1)
        back, front = later(back, *second), later(front, *second)
        far_low, far_high = shift(back[:half], 1), shift(front[half:], -1)
        across = jnp.concatenate([later(far_low, *third), later(far_high, *third)], axis=0)
        whole = jnp.zeros((n_tp,) + shard.shape, shard.dtype)
        for hops, piece in ((0, shard), (chips - 1, back), (1, front), (2, across)):
            place = lax.rem(chip + hops, chips) * CORES
            other = later(swap(piece), *third)
            whole = lax.dynamic_update_slice_in_dim(whole, later(piece, *third)[None], place + core, 0)
            whole = lax.dynamic_update_slice_in_dim(whole, other[None], place + 1 - core, 0)
        return whole

    def per_device(y_one, y_two, dy_one, dy_two, saved_one, saved_two, w_qkv, w_o, w_in, w_out):
        n_layers, width, _, n_heads, size = w_qkv.shape
        n_pairs = saved_one.shape[0]
        me = lax.axis_index("tp")
        plan = Plan(me.reshape(1).astype(jnp.int32), y_one.shape[0])
        w_t = jnp.transpose(w_qkv, (0, 2, 3, 4, 1)).reshape(n_layers, 3 * n_heads * size, width)
        w_o2 = w_o.reshape(n_layers, n_heads * size, width)

        def own(state):
            return lax.dynamic_slice_in_dim(state, me, 1, 0)

        top = n_layers - 1
        dx, parts = mlp_back(plan, y_one, dy_two, None, w_in, w_out, top)
        g_back = scatter(dx)
        g_part = mlp_forward(plan.after(dx), y_one, w_in, w_out, top)
        g_sums = core_sums(g_part)
        d_one = own(dy_one) + rms_pull(own(y_one), later(g_back, g_sums).astype(F32))
        d_shard = d_one.astype(BF16)
        mlp_held = mlp_grads(plan.after(d_shard), parts, dy_two, None, top, n_layers, None)
        g_sum = like_scatter(later(g_sums, d_shard))
        x_two_out = own(y_two)
        wo_all = ring_gather(w_o2[0], (dx,), (g_part,)).reshape(-1, width)
        d_two, attn_held, last = own(dy_two), None, mlp_held[0]

        for layer_pair in reversed(range(n_pairs)):
            s_one, s_two = saved_one[layer_pair], saved_two[layer_pair]
            mid, low = 2 * layer_pair + 1, 2 * layer_pair
            g_part = mlp_forward(plan.after(last), s_one, w_in, w_out, low)
            d_one_bf = gather(d_shard, g_part)
            finish, chip_sums = ring_scatter(g_part)
            mid_back, attn_held, _ = attn_back(
                plan.after(chip_sums), s_two, d_one_bf, w_t, w_o2, mid, n_heads, n_layers, attn_held
            )
            mid_sums = core_sums(mid_back)
            x_two_shard = x_two_out - later(g_sum, mid_sums)
            f_shard = rms_bf(x_two_shard)
            f_in = gather(f_shard)
            mid_sum = like_scatter(later(mid_sums, f_shard))
            f_back, attn_held, _ = attn_back(
                plan, f_in, d_one_bf, w_t, w_o2, mid + 1, n_heads, n_layers, attn_held
            )
            low_two = own(s_two) - finish((f_in,), (f_back,))
            mid_two = d_two + rms_pull(x_two_shard, scatter(f_back).astype(F32))
            d_two = mid_two + rms_pull(own(s_two), later(mid_sum, f_back).astype(F32))
            both_d = gather(jnp.stack([mid_two.astype(BF16), d_two.astype(BF16)], axis=1))
            dx, mid_parts = mlp_back(plan, s_one, both_d, 0, w_in, w_out, mid)
            mid_dx = dx
            dx, low_parts = mlp_back(plan, s_one, both_d, 1, w_in, w_out, low, dx)
            x_two = ring_gather(later(low_two[0], both_d), (mid_dx,), (dx,))
            heads, x_two = attn_forward(plan, x_two, w_t, low, n_heads)
            x_two_shard = low_two
            d_one = d_one + rms_pull(own(s_one), later(scatter(dx), heads).astype(F32))
            if layer_pair:
                d_shard, last = d_one.astype(BF16), dx
                g_sum, x_two_out = jnp.zeros_like(x_two_shard), x_two_shard
                mlp_held = mlp_grads(plan, mid_parts, both_d, 0, mid, n_layers, mlp_held)
                mlp_held = mlp_grads(plan, low_parts, both_d, 1, low, n_layers, mlp_held)
        f_back, attn_held, d_one_full = attn_back(
            plan, x_two, gather(d_one), w_t, w_o2, 0, n_heads, n_layers, attn_held, True
        )
        heads_all = gather(later(heads, d_one), f_back)
        d_two = d_two + rms_pull(x_two_shard, scatter(later(f_back, heads_all)).astype(F32))
        tail = plan.after(f_back)
        mlp_held = mlp_grads(tail, mid_parts, both_d, 0, 1, n_layers, mlp_held)
        mlp_held = mlp_grads(tail, low_parts, both_d, 1, 0, n_layers, mlp_held)
        x_one = project_out(tail, s_one, heads_all, wo_all)
        d_two_full = gather(d_two, x_one, mlp_held[0])
        d_w = jnp.transpose(attn_held[0].reshape(n_layers, 3, n_heads, size, width), (0, 4, 1, 2, 3))
        d_wo = attn_held[1].reshape(n_layers, n_heads, size, width)
        return (x_one, x_two, d_one_full, d_two_full, d_w, d_wo) + tuple(mlp_held)

    return jax.shard_map(
        per_device,
        mesh=mesh,
        in_specs=(act_spec,) * 4 + (saved_spec,) * 2 + weight_specs,
        out_specs=(act_spec,) * 4 + grad_specs,
        check_vma=False,
    )
```

```python
import jax
import jax.numpy as jnp
from jax import lax
from jax.experimental import pallas as pl
from jax.experimental.pallas import tpu as pltpu
from jax.sharding import PartitionSpec as P


EPS = 1e-6
F32, BF16 = jnp.float32, jnp.bfloat16
CORES = 2
STEP = 2
VMEM = 60 * 1024 * 1024


def dot(lhs, rhs, lhs_dim, rhs_dim):
    return lax.dot_general(lhs, rhs, (((lhs_dim,), (rhs_dim,)), ((), ())), preferred_element_type=F32)


def later(value, *others):
    return lax.optimization_barrier((value,) + others)[0]


def rms_scale(state):
    return lax.rsqrt(jnp.mean(state * state, axis=-1, keepdims=True) + EPS)


def rms_bf(state):
    return (state * rms_scale(state)).astype(BF16)


def rms_pull(state, cot):
    scale = rms_scale(state)
    normed = state * scale
    return scale * (cot - normed * jnp.mean(normed * cot, axis=-1, keepdims=True))


class Plan:
    def __init__(self, gate, n_seq):
        self.gate = gate
        self.n_seq = n_seq

    def after(self, *values):
        return Plan(later(self.gate, *values), self.n_seq)

    @staticmethod
    def seqs(array, slot=None):
        rows, cols = array.shape[-2:]
        if array.ndim == 4:
            return pl.BlockSpec((STEP, None, rows, cols), lambda g, gate: (g, slot, 0, 0))
        return pl.BlockSpec((STEP, rows, cols), lambda g, gate: (g, 0, 0))

    @staticmethod
    def layer(index, rows, cols):
        return pl.BlockSpec((None, rows, cols), lambda g, gate: (index, 0, 0))

    def call(self, body, in_specs, out_specs, out_shape, args, flops, aliases=None):
        n_bytes = sum(x.size * x.dtype.itemsize for x in out_shape)
        return pl.pallas_call(
            body,
            grid_spec=pltpu.PrefetchScalarGridSpec(
                num_scalar_prefetch=1, grid=(self.n_seq // STEP,), in_specs=in_specs, out_specs=out_specs
            ),
            out_shape=out_shape,
            input_output_aliases=aliases or {},
            cost_estimate=pl.CostEstimate(flops=int(flops), bytes_accessed=int(n_bytes), transcendentals=0),
            compiler_params=pltpu.CompilerParams(dimension_semantics=("arbitrary",), vmem_limit_bytes=VMEM),
        )(self.gate, *args)


def flat(ref):
    return ref[...].reshape(-1, ref.shape[-1])


def put(ref, value):
    ref[...] = value.astype(ref.dtype).reshape(ref.shape)


def accumulate(pairs):
    @pl.when(pl.program_id(0) == 0)
    def _():
        for ref, value in pairs:
            ref[...] = value

    @pl.when(pl.program_id(0) > 0)
    def _():
        for ref, value in pairs:
            ref[...] += value


def gelu_parts(hidden):
    root = (2.0 / jnp.pi) ** 0.5
    square = hidden * hidden
    bent = jnp.tanh(root * (hidden + 0.044715 * (square * hidden)))
    cdf = 0.5 * (1.0 + bent)
    return hidden * cdf, bent, cdf, root, square


def gelu_slope(hidden):
    act, bent, cdf, root, square = gelu_parts(hidden)
    return act.astype(BF16), cdf + 0.5 * hidden * (1.0 - bent * bent) * (root * (1.0 + 3.0 * 0.044715 * square))


def mlp_forward(plan, state, w_in, w_out, layer, want_out=True, keep=False):
    n_seq, rows, width = state.shape
    ff = w_in.shape[-1]

    def body(gate, x_ref, win_ref, *refs):
        normed = rms_bf(flat(x_ref))
        hidden = dot(normed, win_ref[...], 1, 0)
        if keep:
            act, slope = gelu_slope(hidden)
            for ref, value in zip(refs[-3:], (normed, act, slope)):
                put(ref, value)
        else:
            act = gelu_parts(hidden)[0].astype(BF16)
        if want_out:
            put(refs[1], dot(act, refs[0][...], 1, 0))

    out_shape = [jax.ShapeDtypeStruct(state.shape, F32)] if want_out else []
    if keep:
        out_shape += [jax.ShapeDtypeStruct((n_seq, rows, n), t) for n, t in ((width, BF16), (ff, BF16), (ff, F32))]
    in_specs = [plan.seqs(state), plan.layer(layer, width, ff)] + [plan.layer(layer, ff, width)] * want_out
    return plan.call(
        body,
        in_specs,
        [plan.seqs(x) for x in out_shape],
        out_shape,
        [state, w_in] + [w_out] * want_out,
        (2 + 2 * want_out) * n_seq * rows * width * ff,
    )


def mlp_back_kept(plan, slope, d_out, slot, w_in, w_out, layer, extra=None):
    n_seq, rows, ff = slope.shape
    width = w_in.shape[1]
    n_e = 0 if extra is None else 1

    def body(gate, slope_ref, d_ref, win_ref, wout_ref, *refs):
        dx_ref, dh_ref = refs[n_e:]
        d_hidden = (flat(slope_ref) * dot(flat(d_ref), wout_ref[...], 1, 1)).astype(BF16)
        d_x = dot(d_hidden, win_ref[...], 1, 1)
        if n_e:
            d_x = d_x + flat(refs[0]).astype(F32)
        put(dx_ref, d_x)
        put(dh_ref, d_hidden)

    in_specs = [plan.seqs(slope), plan.seqs(d_out, slot), plan.layer(layer, width, ff), plan.layer(layer, ff, width)]
    args = [slope, d_out, w_in, w_out]
    if n_e:
        in_specs.append(plan.seqs(extra))
        args.append(extra)
    out_shape = [jax.ShapeDtypeStruct((n_seq, rows, width), BF16), jax.ShapeDtypeStruct((n_seq, rows, ff), BF16)]
    return plan.call(body, in_specs, [plan.seqs(x) for x in out_shape], out_shape, args, 4 * n_seq * rows * width * ff)


def mlp_back(plan, state, d_out, slot, w_in, w_out, layer, extra=None):
    n_seq, rows, width = state.shape
    ff = w_in.shape[-1]
    n_e = 0 if extra is None else 1

    def body(gate, x_ref, d_ref, win_ref, wout_ref, *refs):
        dx_ref, a_ref, act_ref, dh_ref = refs[n_e:]
        normed = rms_bf(flat(x_ref))
        hidden = dot(normed, win_ref[...], 1, 0)
        d_act = dot(flat(d_ref).astype(BF16), wout_ref[...], 1, 1)
        act, bent, cdf, root, square = gelu_parts(hidden)
        slope = cdf + 0.5 * hidden * (1.0 - bent * bent) * (root * (1.0 + 3.0 * 0.044715 * square))
        d_hidden = (slope * d_act).astype(BF16)
        d_x = dot(d_hidden, win_ref[...], 1, 1)
        if n_e:
            d_x = d_x + flat(refs[0]).astype(F32)
        put(dx_ref, d_x)
        put(a_ref, normed)
        put(act_ref, act)
        put(dh_ref, d_hidden)

    in_specs = [plan.seqs(state), plan.seqs(d_out, slot), plan.layer(layer, width, ff), plan.layer(layer, ff, width)]
    args = [state, d_out, w_in, w_out]
    if n_e:
        in_specs.append(plan.seqs(extra))
        args.append(extra)
    wide = jax.ShapeDtypeStruct((n_seq, rows, width), BF16)
    narrow = jax.ShapeDtypeStruct((n_seq, rows, ff), BF16)
    out_shape = [wide, wide, narrow, narrow]
    outs = plan.call(body, in_specs, [plan.seqs(x) for x in out_shape], out_shape, args, 6 * n_seq * rows * width * ff)
    return outs[0], tuple(outs[1:])


def mlp_grads(plan, parts, d_out, slot, layer, n_layers, held):
    normed, act, d_hidden = parts
    n_seq, rows, width = normed.shape
    ff = act.shape[-1]
    n_held = 0 if held is None else 2

    def body(gate, a_ref, act_ref, dh_ref, d_ref, *refs):
        dwin_ref, dwout_ref = refs[n_held:]
        d_win = dot(flat(a_ref), flat(dh_ref), 0, 0)
        d_wout = dot(flat(act_ref), flat(d_ref).astype(BF16), 0, 0)
        accumulate([(dwin_ref, d_win), (dwout_ref, d_wout)])

    in_specs = [plan.seqs(normed), plan.seqs(act), plan.seqs(d_hidden), plan.seqs(d_out, slot)]
    args = [normed, act, d_hidden, d_out]
    aliases = {}
    if n_held:
        aliases = {len(args) + 1 + i: i for i in range(n_held)}
        in_specs += [pl.BlockSpec(memory_space=pl.ANY)] * n_held
        args += list(held)
    return plan.call(
        body,
        in_specs,
        [plan.layer(layer, width, ff), plan.layer(layer, ff, width)],
        [jax.ShapeDtypeStruct((n_layers, width, ff), F32), jax.ShapeDtypeStruct((n_layers, ff, width), F32)],
        args,
        4 * n_seq * rows * width * ff,
        aliases,
    )


def softmax(scores):
    powers = jnp.exp(scores - jnp.max(scores, axis=-1, keepdims=True))
    return powers / jnp.sum(powers, axis=-1, keepdims=True)


def cut(value, row, size, col, rows):
    return value[row * size :][:size][:, col * rows :][:, :rows].astype(BF16)


def attn_forward(plan, state, w_t, layer, n_heads):
    n_seq, rows, width = state.shape
    depth = w_t.shape[1]
    size = depth // 3 // n_heads

    def body(gate, x_ref, w_ref, out_ref, state_ref):
        state_ref[...] = x_ref[...]
        qkv = dot(w_ref[...], rms_bf(flat(x_ref)), 1, 1)
        cols = []
        for col in range(STEP):
            outs = []
            for head in range(n_heads):
                q, k, v = (cut(qkv, kind * n_heads + head, size, col, rows) for kind in range(3))
                probs = softmax(dot(q, k, 0, 0) * size ** -0.5).astype(BF16)
                outs.append(dot(v, probs, 1, 1))
            cols.append(jnp.concatenate(outs, axis=0))
        out_ref[...] = jnp.concatenate(cols, axis=1).astype(BF16)

    return plan.call(
        body,
        [plan.seqs(state), plan.layer(layer, depth, width)],
        [pl.BlockSpec((depth // 3, STEP * rows), lambda g, gate: (0, g)), plan.seqs(state)],
        [jax.ShapeDtypeStruct((depth // 3, n_seq * rows), BF16), jax.ShapeDtypeStruct(state.shape, F32)],
        (state, w_t),
        2 * n_seq * rows * width * depth,
    )


def attn_back(plan, state, d_out, w_t, w_o, layer, n_heads, n_layers, held, keep_d=False):
    n_seq, rows, width = state.shape
    depth = w_t.shape[1]
    size = depth // 3 // n_heads
    n_held = 0 if held is None else 2

    def body(gate, x_ref, d_ref, w_ref, wo_ref, *refs):
        dx_ref, dw_ref, dwo_ref = refs[n_held:][:3]
        normed = flat(x_ref) if x_ref.dtype == BF16 else rms_bf(flat(x_ref))
        d_bf = flat(d_ref).astype(BF16)
        if keep_d:
            refs[-1][...] = d_ref[...]
        qkv = dot(w_ref[...], normed, 1, 1)
        d_heads = dot(wo_ref[...], d_bf, 1, 1)
        out_cols, d_cols = [], []
        for col in range(STEP):
            outs, d_parts = [], [[], [], []]
            for head in range(n_heads):
                q, k, v = (cut(qkv, kind * n_heads + head, size, col, rows) for kind in range(3))
                d_head = cut(d_heads, head, size, col, rows)
                probs = softmax(dot(q, k, 0, 0) * size ** -0.5)
                probs_bf = probs.astype(BF16)
                outs.append(dot(v, probs_bf, 1, 1))
                d_probs = dot(d_head, v, 0, 0)
                d_scores = probs * (d_probs - jnp.sum(d_probs * probs, axis=-1, keepdims=True)) * size ** -0.5
                d_scores = d_scores.astype(BF16)
                d_parts[0].append(dot(k, d_scores, 1, 1))
                d_parts[1].append(dot(q, d_scores, 1, 0))
                d_parts[2].append(dot(d_head, probs_bf, 1, 0))
            out_cols.append(jnp.concatenate(outs, axis=0))
            d_cols.append(jnp.concatenate(d_parts[0] + d_parts[1] + d_parts[2], axis=0))
        d_qkv = jnp.concatenate(d_cols, axis=1).astype(BF16)
        put(dx_ref, dot(d_qkv, w_ref[...], 0, 0))
        heads = jnp.concatenate(out_cols, axis=1).astype(BF16)
        accumulate([(dw_ref, dot(d_qkv, normed, 1, 0)), (dwo_ref, dot(heads, d_bf, 1, 0))])

    in_specs = [plan.seqs(state), plan.seqs(d_out), plan.layer(layer, depth, width), plan.layer(layer, depth // 3, width)]
    args = [state, d_out, w_t, w_o]
    aliases = {}
    if n_held:
        aliases = {len(args) + 1 + i: 1 + i for i in range(n_held)}
        in_specs += [pl.BlockSpec(memory_space=pl.ANY)] * n_held
        args += list(held)
    out_specs = [plan.seqs(state), plan.layer(layer, depth, width), plan.layer(layer, depth // 3, width)]
    out_shape = [
        jax.ShapeDtypeStruct(state.shape, BF16),
        jax.ShapeDtypeStruct((n_layers, depth, width), F32),
        jax.ShapeDtypeStruct((n_layers, depth // 3, width), F32),
    ]
    if keep_d:
        out_specs.append(plan.seqs(d_out))
        out_shape.append(jax.ShapeDtypeStruct(d_out.shape, d_out.dtype))
    outs = plan.call(body, in_specs, out_specs, out_shape, args, 8 * n_seq * rows * width * depth, aliases)
    return outs[0], tuple(outs[1:3]), (outs[3] if keep_d else None)


def project_out(plan, base, heads, w_o):
    n_seq, rows, width = base.shape
    depth = heads.shape[0]

    def body(gate, x_ref, h_ref, w_ref, out_ref):
        put(out_ref, flat(x_ref) - dot(h_ref[...], w_ref[...], 0, 0))

    return plan.call(
        body,
        [
            plan.seqs(base),
            pl.BlockSpec((depth, STEP * rows), lambda g, gate: (0, g)),
            pl.BlockSpec((depth, width), lambda g, gate: (0, 0)),
        ],
        [plan.seqs(base)],
        [jax.ShapeDtypeStruct(base.shape, F32)],
        (base, heads, w_o),
        2 * n_seq * rows * width * depth,
    )[0]


def solution(mesh):
    act_spec = P("dp", None, None)
    saved_spec = P(None, "dp", None, None)
    weight_specs = (P(None, None, None, "tp", None), P(None, "tp", None, None), P(None, None, "tp"), P(None, "tp", None))
    grad_specs = (P("dp", None, None, "tp", None), P("dp", "tp", None, None), P("dp", None, "tp"), P("dp", "tp", None))

    def scatter(part):
        return lax.psum_scatter(part, "tp", scatter_dimension=0, tiled=True)

    def gather(shard, *others):
        return later(lax.all_gather(shard, "tp", axis=0, tiled=True), *others)

    n_tp = mesh.shape["tp"]
    chips = n_tp // CORES

    def shift(value, hops):
        pairs = [(i, (i // CORES + hops) % chips * CORES + i % CORES) for i in range(n_tp)]
        return lax.ppermute(value, "tp", pairs)

    def swap(value):
        return lax.ppermute(value, "tp", [(i, i + 1 - 2 * (i % CORES)) for i in range(n_tp)])

    def core_sums(part):
        core = lax.rem(lax.axis_index("tp"), CORES)
        split = part.reshape((chips, CORES) + part.shape[1:])
        far = swap(lax.dynamic_index_in_dim(split, 1 - core, 1, False))
        return (lax.dynamic_index_in_dim(split, core, 1, False).astype(F32) + far.astype(F32)).astype(part.dtype)

    def like_scatter(sums):
        alike = [list(range(core, n_tp, CORES)) for core in range(CORES)]
        return lax.psum_scatter(sums, "tp", scatter_dimension=0, axis_index_groups=alike, tiled=True)

    def ring_scatter(part):
        chip = lax.div(lax.axis_index("tp"), CORES)
        half = part.shape[1] // 2
        mine = core_sums(part)
        ahead, across, behind, here = (
            lax.dynamic_index_in_dim(mine, lax.rem(chip + hops, chips), 0, False) for hops in (1, 2, 3, 0)
        )
        from_back, from_front = shift(across[:half], 1), shift(across[half:], -1)
        back_low, front_high = shift(ahead[half:], 1), shift(behind[:half], -1)

        def finish(second, third):
            back_high = shift(ahead[:half] + later(from_back, *second), 1)
            front_low = shift(behind[half:] + later(from_front, *second), -1)
            high = later(back_high, *third) + front_high
            low = later(front_low, *third) + back_low
            return (here + jnp.concatenate([high, low], axis=0))[None]

        return finish, mine

    def ring_gather(shard, second, third):
        chip, core = lax.div(lax.axis_index("tp"), CORES), lax.rem(lax.axis_index("tp"), CORES)
        rows = shard.shape[0]
        half = rows // 2
        back, front = shift(shard, 1), shift(shard, -1)
        back, front = later(back, *second), later(front, *second)
        far_low, far_high = shift(back[:half], 1), shift(front[half:], -1)
        across = jnp.concatenate([later(far_low, *third), later(far_high, *third)], axis=0)
        whole = jnp.zeros((n_tp,) + shard.shape, shard.dtype)
        for hops, piece in ((0, shard), (chips - 1, back), (1, front), (2, across)):
            place = lax.rem(chip + hops, chips) * CORES
            other = later(swap(piece), *third)
            whole = lax.dynamic_update_slice_in_dim(whole, later(piece, *third)[None], place + core, 0)
            whole = lax.dynamic_update_slice_in_dim(whole, other[None], place + 1 - core, 0)
        return whole

    def per_device(y_one, y_two, dy_one, dy_two, saved_one, saved_two, w_qkv, w_o, w_in, w_out):
        n_layers, width, _, n_heads, size = w_qkv.shape
        n_pairs = saved_one.shape[0]
        me = lax.axis_index("tp")
        plan = Plan(me.reshape(1).astype(jnp.int32), y_one.shape[0])
        w_t = jnp.transpose(w_qkv, (0, 2, 3, 4, 1)).reshape(n_layers, 3 * n_heads * size, width)
        w_o2 = w_o.reshape(n_layers, n_heads * size, width)

        def own(state):
            return lax.dynamic_slice_in_dim(state, me, 1, 0)

        top = n_layers - 1
        dx, parts = mlp_back(plan, y_one, dy_two, None, w_in, w_out, top)
        g_back = scatter(dx)
        (g_part,) = mlp_forward(plan.after(dx), y_one, w_in, w_out, top)
        g_sums = core_sums(g_part)
        d_one = own(dy_one) + rms_pull(own(y_one), later(g_back, g_part).astype(F32))
        d_shard = d_one.astype(BF16)
        mlp_held = mlp_grads(plan.after(d_shard), parts, dy_two, None, top, n_layers, None)
        g_sum = like_scatter(later(g_sums, d_shard))
        x_two_out = own(y_two)
        wo_all = ring_gather(w_o2[0], (dx,), (g_part,)).reshape(-1, width)
        d_two, attn_held, last = own(dy_two), None, mlp_held[0]

        for layer_pair in reversed(range(n_pairs)):
            s_one, s_two = saved_one[layer_pair], saved_two[layer_pair]
            mid, low = 2 * layer_pair + 1, 2 * layer_pair
            g_part, normed, low_act, low_slope = mlp_forward(plan.after(last), s_one, w_in, w_out, low, keep=True)
            d_one_bf = gather(d_shard, g_part)
            finish, chip_sums = ring_scatter(g_part)
            mid_back, attn_held, _ = attn_back(
                plan.after(chip_sums), s_two, d_one_bf, w_t, w_o2, mid, n_heads, n_layers, attn_held
            )
            mid_sums = core_sums(mid_back)
            x_two_shard = x_two_out - later(g_sum, mid_sums)
            f_shard = rms_bf(x_two_shard)
            f_in = gather(f_shard)
            mid_sum = like_scatter(later(mid_sums, f_shard))
            _, mid_act, mid_slope = mlp_forward(plan.after(f_shard), s_one, w_in, w_out, mid, want_out=False, keep=True)
            f_in = later(f_in, mid_slope)
            f_back, attn_held, _ = attn_back(
                plan, f_in, d_one_bf, w_t, w_o2, mid + 1, n_heads, n_layers, attn_held
            )
            low_two = own(s_two) - finish((f_in,), (f_back,))
            mid_two = d_two + rms_pull(x_two_shard, scatter(f_back).astype(F32))
            d_two = mid_two + rms_pull(own(s_two), later(mid_sum, f_back).astype(F32))
            both_d = gather(jnp.stack([mid_two.astype(BF16), d_two.astype(BF16)], axis=1))
            dx, mid_dh = mlp_back_kept(plan, mid_slope, both_d, 0, w_in, w_out, mid)
            dx, low_dh = mlp_back_kept(plan, low_slope, both_d, 1, w_in, w_out, low, dx)
            dx_sum = scatter(dx)
            mid_parts, low_parts = (normed, mid_act, mid_dh), (normed, low_act, low_dh)
            mlp_held = mlp_grads(plan.after(dx), mid_parts, both_d, 0, mid, n_layers, mlp_held)
            x_two = ring_gather(later(low_two[0], both_d), (dx,), (mlp_held[0],))
            x_two_shard = low_two
            d_one = d_one + rms_pull(own(s_one), later(dx_sum, mlp_held[0]).astype(F32))
            heads, x_two = attn_forward(plan.after(d_one), x_two, w_t, low, n_heads)
            if layer_pair:
                d_shard, last = d_one.astype(BF16), dx
                g_sum, x_two_out = jnp.zeros_like(x_two_shard), x_two_shard
                mlp_held = mlp_grads(plan, low_parts, both_d, 1, low, n_layers, mlp_held)
        f_back, attn_held, d_one_full = attn_back(
            plan, x_two, gather(d_one, heads), w_t, w_o2, 0, n_heads, n_layers, attn_held, True
        )
        heads_all = gather(later(heads, d_one), f_back)
        d_two = d_two + rms_pull(x_two_shard, scatter(later(f_back, heads_all)).astype(F32))
        tail = plan.after(f_back)
        mlp_held = mlp_grads(tail, low_parts, both_d, 1, 0, n_layers, mlp_held)
        x_one = project_out(tail, s_one, heads_all, wo_all)
        d_two_full = gather(d_two, x_one, mlp_held[0])
        d_w = jnp.transpose(attn_held[0].reshape(n_layers, 3, n_heads, size, width), (0, 4, 1, 2, 3))
        d_wo = attn_held[1].reshape(n_layers, n_heads, size, width)
        return (x_one, x_two, d_one_full, d_two_full, d_w, d_wo) + tuple(mlp_held)

    return jax.shard_map(
        per_device,
        mesh=mesh,
        in_specs=(act_spec,) * 4 + (saved_spec,) * 2 + weight_specs,
        out_specs=(act_spec,) * 4 + grad_specs,
        check_vma=False,
    )
```

```python
import jax
import jax.numpy as jnp
from jax import lax
from jax.experimental import pallas as pl
from jax.experimental.pallas import tpu as pltpu
from jax.sharding import PartitionSpec as P


EPS = 1e-6
F32, BF16 = jnp.float32, jnp.bfloat16
CORES = 2
STEP = 2
VMEM = 60 * 1024 * 1024


def dot(lhs, rhs, lhs_dim, rhs_dim):
    return lax.dot_general(lhs, rhs, (((lhs_dim,), (rhs_dim,)), ((), ())), preferred_element_type=F32)


def later(value, *others):
    return lax.optimization_barrier((value,) + others)[0]


def rms_scale(state):
    return lax.rsqrt(jnp.mean(state * state, axis=-1, keepdims=True) + EPS)


def rms_bf(state):
    return (state * rms_scale(state)).astype(BF16)


def rms_pull(state, cot):
    scale = rms_scale(state)
    normed = state * scale
    return scale * (cot - normed * jnp.mean(normed * cot, axis=-1, keepdims=True))


class Plan:
    def __init__(self, gate, n_seq):
        self.gate = gate
        self.n_seq = n_seq

    def after(self, *values):
        return Plan(later(self.gate, *values), self.n_seq)

    @staticmethod
    def seqs(array, slot=None):
        rows, cols = array.shape[-2:]
        if array.ndim == 4:
            return pl.BlockSpec((STEP, None, rows, cols), lambda g, gate: (g, slot, 0, 0))
        return pl.BlockSpec((STEP, rows, cols), lambda g, gate: (g, 0, 0))

    @staticmethod
    def layer(index, rows, cols):
        return pl.BlockSpec((None, rows, cols), lambda g, gate: (index, 0, 0))

    def call(self, body, in_specs, out_specs, out_shape, args, flops, aliases=None):
        n_bytes = sum(x.size * x.dtype.itemsize for x in out_shape)
        return pl.pallas_call(
            body,
            grid_spec=pltpu.PrefetchScalarGridSpec(
                num_scalar_prefetch=1, grid=(self.n_seq // STEP,), in_specs=in_specs, out_specs=out_specs
            ),
            out_shape=out_shape,
            input_output_aliases=aliases or {},
            cost_estimate=pl.CostEstimate(flops=int(flops), bytes_accessed=int(n_bytes), transcendentals=0),
            compiler_params=pltpu.CompilerParams(dimension_semantics=("arbitrary",), vmem_limit_bytes=VMEM),
        )(self.gate, *args)


def flat(ref):
    return ref[...].reshape(-1, ref.shape[-1])


def put(ref, value):
    ref[...] = value.astype(ref.dtype).reshape(ref.shape)


def accumulate(pairs):
    @pl.when(pl.program_id(0) == 0)
    def _():
        for ref, value in pairs:
            ref[...] = value

    @pl.when(pl.program_id(0) > 0)
    def _():
        for ref, value in pairs:
            ref[...] += value


def gelu_parts(hidden):
    root = (2.0 / jnp.pi) ** 0.5
    square = hidden * hidden
    bent = jnp.tanh(root * (hidden + 0.044715 * (square * hidden)))
    cdf = 0.5 * (1.0 + bent)
    return hidden * cdf, bent, cdf, root, square


def gelu_slope(hidden):
    act, bent, cdf, root, square = gelu_parts(hidden)
    return act.astype(BF16), cdf + 0.5 * hidden * (1.0 - bent * bent) * (root * (1.0 + 3.0 * 0.044715 * square))


def mlp_forward(plan, state, w_in, w_out, layer, want_out=True, keep=False):
    n_seq, rows, width = state.shape
    ff = w_in.shape[-1]

    def body(gate, x_ref, win_ref, *refs):
        normed = rms_bf(flat(x_ref))
        hidden = dot(normed, win_ref[...], 1, 0)
        if keep:
            act, slope = gelu_slope(hidden)
            for ref, value in zip(refs[-3:], (normed, act, slope)):
                put(ref, value)
        else:
            act = gelu_parts(hidden)[0].astype(BF16)
        if want_out:
            put(refs[1], dot(act, refs[0][...], 1, 0))

    out_shape = [jax.ShapeDtypeStruct(state.shape, F32)] if want_out else []
    if keep:
        out_shape += [jax.ShapeDtypeStruct((n_seq, rows, n), t) for n, t in ((width, BF16), (ff, BF16), (ff, F32))]
    in_specs = [plan.seqs(state), plan.layer(layer, width, ff)] + [plan.layer(layer, ff, width)] * want_out
    return plan.call(
        body,
        in_specs,
        [plan.seqs(x) for x in out_shape],
        out_shape,
        [state, w_in] + [w_out] * want_out,
        (2 + 2 * want_out) * n_seq * rows * width * ff,
    )


def mlp_back_kept(plan, slope, d_out, slot, w_in, w_out, layer, extra=None):
    n_seq, rows, ff = slope.shape
    width = w_in.shape[1]
    n_e = 0 if extra is None else 1

    def body(gate, slope_ref, d_ref, win_ref, wout_ref, *refs):
        dx_ref, dh_ref = refs[n_e:]
        d_hidden = (flat(slope_ref) * dot(flat(d_ref), wout_ref[...], 1, 1)).astype(BF16)
        d_x = dot(d_hidden, win_ref[...], 1, 1)
        if n_e:
            d_x = d_x + flat(refs[0]).astype(F32)
        put(dx_ref, d_x)
        put(dh_ref, d_hidden)

    in_specs = [plan.seqs(slope), plan.seqs(d_out, slot), plan.layer(layer, width, ff), plan.layer(layer, ff, width)]
    args = [slope, d_out, w_in, w_out]
    if n_e:
        in_specs.append(plan.seqs(extra))
        args.append(extra)
    out_shape = [jax.ShapeDtypeStruct((n_seq, rows, width), BF16), jax.ShapeDtypeStruct((n_seq, rows, ff), BF16)]
    return plan.call(body, in_specs, [plan.seqs(x) for x in out_shape], out_shape, args, 4 * n_seq * rows * width * ff)


def mlp_back(plan, state, d_out, slot, w_in, w_out, layer, extra=None):
    n_seq, rows, width = state.shape
    ff = w_in.shape[-1]
    n_e = 0 if extra is None else 1

    def body(gate, x_ref, d_ref, win_ref, wout_ref, *refs):
        dx_ref, a_ref, act_ref, dh_ref = refs[n_e:]
        normed = rms_bf(flat(x_ref))
        hidden = dot(normed, win_ref[...], 1, 0)
        d_act = dot(flat(d_ref).astype(BF16), wout_ref[...], 1, 1)
        act, bent, cdf, root, square = gelu_parts(hidden)
        slope = cdf + 0.5 * hidden * (1.0 - bent * bent) * (root * (1.0 + 3.0 * 0.044715 * square))
        d_hidden = (slope * d_act).astype(BF16)
        d_x = dot(d_hidden, win_ref[...], 1, 1)
        if n_e:
            d_x = d_x + flat(refs[0]).astype(F32)
        put(dx_ref, d_x)
        put(a_ref, normed)
        put(act_ref, act)
        put(dh_ref, d_hidden)

    in_specs = [plan.seqs(state), plan.seqs(d_out, slot), plan.layer(layer, width, ff), plan.layer(layer, ff, width)]
    args = [state, d_out, w_in, w_out]
    if n_e:
        in_specs.append(plan.seqs(extra))
        args.append(extra)
    wide = jax.ShapeDtypeStruct((n_seq, rows, width), BF16)
    narrow = jax.ShapeDtypeStruct((n_seq, rows, ff), BF16)
    out_shape = [wide, wide, narrow, narrow]
    outs = plan.call(body, in_specs, [plan.seqs(x) for x in out_shape], out_shape, args, 6 * n_seq * rows * width * ff)
    return outs[0], tuple(outs[1:])


def mlp_grads(plan, parts, d_out, slot, layer, n_layers, held):
    normed, act, d_hidden = parts
    n_seq, rows, width = normed.shape
    ff = act.shape[-1]
    n_held = 0 if held is None else 2

    def body(gate, a_ref, act_ref, dh_ref, d_ref, *refs):
        dwin_ref, dwout_ref = refs[n_held:]
        d_win = dot(flat(a_ref), flat(dh_ref), 0, 0)
        d_wout = dot(flat(act_ref), flat(d_ref).astype(BF16), 0, 0)
        accumulate([(dwin_ref, d_win), (dwout_ref, d_wout)])

    in_specs = [plan.seqs(normed), plan.seqs(act), plan.seqs(d_hidden), plan.seqs(d_out, slot)]
    args = [normed, act, d_hidden, d_out]
    aliases = {}
    if n_held:
        aliases = {len(args) + 1 + i: i for i in range(n_held)}
        in_specs += [pl.BlockSpec(memory_space=pl.ANY)] * n_held
        args += list(held)
    return plan.call(
        body,
        in_specs,
        [plan.layer(layer, width, ff), plan.layer(layer, ff, width)],
        [jax.ShapeDtypeStruct((n_layers, width, ff), F32), jax.ShapeDtypeStruct((n_layers, ff, width), F32)],
        args,
        4 * n_seq * rows * width * ff,
        aliases,
    )


def softmax(scores):
    powers = jnp.exp(scores - jnp.max(scores, axis=-1, keepdims=True))
    return powers / jnp.sum(powers, axis=-1, keepdims=True)


def cut(value, row, size, col, rows):
    return value[row * size :][:size][:, col * rows :][:, :rows].astype(BF16)


def attn_forward(plan, state, w_t, layer, n_heads):
    n_seq, rows, width = state.shape
    depth = w_t.shape[1]
    size = depth // 3 // n_heads

    def body(gate, x_ref, w_ref, out_ref, state_ref):
        state_ref[...] = x_ref[...]
        qkv = dot(w_ref[...], rms_bf(flat(x_ref)), 1, 1)
        cols = []
        for col in range(STEP):
            outs = []
            for head in range(n_heads):
                q, k, v = (cut(qkv, kind * n_heads + head, size, col, rows) for kind in range(3))
                probs = softmax(dot(q, k, 0, 0) * size ** -0.5).astype(BF16)
                outs.append(dot(v, probs, 1, 1))
            cols.append(jnp.concatenate(outs, axis=0))
        out_ref[...] = jnp.concatenate(cols, axis=1).astype(BF16)

    return plan.call(
        body,
        [plan.seqs(state), plan.layer(layer, depth, width)],
        [pl.BlockSpec((depth // 3, STEP * rows), lambda g, gate: (0, g)), plan.seqs(state)],
        [jax.ShapeDtypeStruct((depth // 3, n_seq * rows), BF16), jax.ShapeDtypeStruct(state.shape, F32)],
        (state, w_t),
        2 * n_seq * rows * width * depth,
    )


def attn_back(plan, state, d_out, w_t, w_o, layer, n_heads, n_layers, held, keep_d=False):
    n_seq, rows, width = state.shape
    depth = w_t.shape[1]
    size = depth // 3 // n_heads
    n_held = 0 if held is None else 2

    def body(gate, x_ref, d_ref, w_ref, wo_ref, *refs):
        dx_ref, dw_ref, dwo_ref = refs[n_held:][:3]
        normed = flat(x_ref) if x_ref.dtype == BF16 else rms_bf(flat(x_ref))
        d_bf = flat(d_ref).astype(BF16)
        if keep_d:
            refs[-1][...] = d_ref[...]
        qkv = dot(w_ref[...], normed, 1, 1)
        d_heads = dot(wo_ref[...], d_bf, 1, 1)
        out_cols, d_cols = [], []
        for col in range(STEP):
            outs, d_parts = [], [[], [], []]
            for head in range(n_heads):
                q, k, v = (cut(qkv, kind * n_heads + head, size, col, rows) for kind in range(3))
                d_head = cut(d_heads, head, size, col, rows)
                probs = softmax(dot(q, k, 0, 0) * size ** -0.5)
                probs_bf = probs.astype(BF16)
                outs.append(dot(v, probs_bf, 1, 1))
                d_probs = dot(d_head, v, 0, 0)
                d_scores = probs * (d_probs - jnp.sum(d_probs * probs, axis=-1, keepdims=True)) * size ** -0.5
                d_scores = d_scores.astype(BF16)
                d_parts[0].append(dot(k, d_scores, 1, 1))
                d_parts[1].append(dot(q, d_scores, 1, 0))
                d_parts[2].append(dot(d_head, probs_bf, 1, 0))
            out_cols.append(jnp.concatenate(outs, axis=0))
            d_cols.append(jnp.concatenate(d_parts[0] + d_parts[1] + d_parts[2], axis=0))
        d_qkv = jnp.concatenate(d_cols, axis=1).astype(BF16)
        put(dx_ref, dot(d_qkv, w_ref[...], 0, 0))
        heads = jnp.concatenate(out_cols, axis=1).astype(BF16)
        accumulate([(dw_ref, dot(d_qkv, normed, 1, 0)), (dwo_ref, dot(heads, d_bf, 1, 0))])

    in_specs = [plan.seqs(state), plan.seqs(d_out), plan.layer(layer, depth, width), plan.layer(layer, depth // 3, width)]
    args = [state, d_out, w_t, w_o]
    aliases = {}
    if n_held:
        aliases = {len(args) + 1 + i: 1 + i for i in range(n_held)}
        in_specs += [pl.BlockSpec(memory_space=pl.ANY)] * n_held
        args += list(held)
    out_specs = [plan.seqs(state), plan.layer(layer, depth, width), plan.layer(layer, depth // 3, width)]
    out_shape = [
        jax.ShapeDtypeStruct(state.shape, BF16),
        jax.ShapeDtypeStruct((n_layers, depth, width), F32),
        jax.ShapeDtypeStruct((n_layers, depth // 3, width), F32),
    ]
    if keep_d:
        out_specs.append(plan.seqs(d_out))
        out_shape.append(jax.ShapeDtypeStruct(d_out.shape, d_out.dtype))
    outs = plan.call(body, in_specs, out_specs, out_shape, args, 8 * n_seq * rows * width * depth, aliases)
    return outs[0], tuple(outs[1:3]), (outs[3] if keep_d else None)


def project_out(plan, base, heads, w_o):
    n_seq, rows, width = base.shape
    depth = heads.shape[0]

    def body(gate, x_ref, h_ref, w_ref, out_ref):
        put(out_ref, flat(x_ref) - dot(h_ref[...], w_ref[...], 0, 0))

    return plan.call(
        body,
        [
            plan.seqs(base),
            pl.BlockSpec((depth, STEP * rows), lambda g, gate: (0, g)),
            pl.BlockSpec((depth, width), lambda g, gate: (0, 0)),
        ],
        [plan.seqs(base)],
        [jax.ShapeDtypeStruct(base.shape, F32)],
        (base, heads, w_o),
        2 * n_seq * rows * width * depth,
    )[0]


def solution(mesh):
    act_spec = P("dp", None, None)
    saved_spec = P(None, "dp", None, None)
    weight_specs = (P(None, None, None, "tp", None), P(None, "tp", None, None), P(None, None, "tp"), P(None, "tp", None))
    grad_specs = (P("dp", None, None, "tp", None), P("dp", "tp", None, None), P("dp", None, "tp"), P("dp", "tp", None))

    def scatter(part):
        return lax.psum_scatter(part, "tp", scatter_dimension=0, tiled=True)

    def gather(shard, *others):
        return later(lax.all_gather(shard, "tp", axis=0, tiled=True), *others)

    n_tp = mesh.shape["tp"]
    chips = n_tp // CORES

    def shift(value, hops):
        pairs = [(i, (i // CORES + hops) % chips * CORES + i % CORES) for i in range(n_tp)]
        return lax.ppermute(value, "tp", pairs)

    def swap(value):
        return lax.ppermute(value, "tp", [(i, i + 1 - 2 * (i % CORES)) for i in range(n_tp)])

    def core_sums(part):
        core = lax.rem(lax.axis_index("tp"), CORES)
        split = part.reshape((chips, CORES) + part.shape[1:])
        far = swap(lax.dynamic_index_in_dim(split, 1 - core, 1, False))
        return (lax.dynamic_index_in_dim(split, core, 1, False).astype(F32) + far.astype(F32)).astype(part.dtype)

    def like_scatter(sums):
        alike = [list(range(core, n_tp, CORES)) for core in range(CORES)]
        return lax.psum_scatter(sums, "tp", scatter_dimension=0, axis_index_groups=alike, tiled=True)

    def ring_scatter(part):
        chip = lax.div(lax.axis_index("tp"), CORES)
        half = part.shape[1] // 2
        mine = core_sums(part)
        ahead, across, behind, here = (
            lax.dynamic_index_in_dim(mine, lax.rem(chip + hops, chips), 0, False) for hops in (1, 2, 3, 0)
        )
        from_back, from_front = shift(across[:half], 1), shift(across[half:], -1)
        back_low, front_high = shift(ahead[half:], 1), shift(behind[:half], -1)

        def finish(second, third):
            back_high = shift(ahead[:half] + later(from_back, *second), 1)
            front_low = shift(behind[half:] + later(from_front, *second), -1)
            high = later(back_high, *third) + front_high
            low = later(front_low, *third) + back_low
            return (here + jnp.concatenate([high, low], axis=0))[None]

        return finish, mine

    def ring_gather(shard, second, third):
        chip, core = lax.div(lax.axis_index("tp"), CORES), lax.rem(lax.axis_index("tp"), CORES)
        rows = shard.shape[0]
        half = rows // 2
        back, front = shift(shard, 1), shift(shard, -1)
        back, front = later(back, *second), later(front, *second)
        far_low, far_high = shift(back[:half], 1), shift(front[half:], -1)
        across = jnp.concatenate([later(far_low, *third), later(far_high, *third)], axis=0)
        whole = jnp.zeros((n_tp,) + shard.shape, shard.dtype)
        for hops, piece in ((0, shard), (chips - 1, back), (1, front), (2, across)):
            place = lax.rem(chip + hops, chips) * CORES
            other = later(swap(piece), *third)
            whole = lax.dynamic_update_slice_in_dim(whole, later(piece, *third)[None], place + core, 0)
            whole = lax.dynamic_update_slice_in_dim(whole, other[None], place + 1 - core, 0)
        return whole

    def per_device(y_one, y_two, dy_one, dy_two, saved_one, saved_two, w_qkv, w_o, w_in, w_out):
        n_layers, width, _, n_heads, size = w_qkv.shape
        n_pairs = saved_one.shape[0]
        me = lax.axis_index("tp")
        plan = Plan(me.reshape(1).astype(jnp.int32), y_one.shape[0])
        w_t = jnp.transpose(w_qkv, (0, 2, 3, 4, 1)).reshape(n_layers, 3 * n_heads * size, width)
        w_o2 = w_o.reshape(n_layers, n_heads * size, width)

        def own(state):
            return lax.dynamic_slice_in_dim(state, me, 1, 0)

        top = n_layers - 1
        dx, parts = mlp_back(plan, y_one, dy_two, None, w_in, w_out, top)
        g_back = scatter(dx)
        (g_part,) = mlp_forward(plan.after(dx), y_one, w_in, w_out, top)
        g_sums = core_sums(g_part)
        d_one = own(dy_one) + rms_pull(own(y_one), later(g_back, g_part).astype(F32))
        d_shard = d_one.astype(BF16)
        g_sum = like_scatter(later(g_sums, d_shard))
        x_two_out = own(y_two)
        wo_all = ring_gather(w_o2[0], (dx,), (g_part,)).reshape(-1, width)
        d_two, attn_held, last, mlp_held = own(dy_two), None, g_sums, None

        for layer_pair in reversed(range(n_pairs)):
            s_one, s_two = saved_one[layer_pair], saved_two[layer_pair]
            mid, low = 2 * layer_pair + 1, 2 * layer_pair
            g_part, normed, low_act, low_slope = mlp_forward(
                plan.after(last, d_shard), s_one, w_in, w_out, low, keep=True
            )
            d_one_bf = gather(d_shard, g_part)
            finish, chip_sums = ring_scatter(g_part)
            mid_back, attn_held, _ = attn_back(
                plan.after(chip_sums), s_two, d_one_bf, w_t, w_o2, mid, n_heads, n_layers, attn_held
            )
            mid_sums = core_sums(mid_back)
            x_two_shard = x_two_out - later(g_sum, mid_sums)
            f_shard = rms_bf(x_two_shard)
            f_in = gather(f_shard)
            mid_sum = like_scatter(later(mid_sums, f_shard))
            _, mid_act, mid_slope = mlp_forward(plan.after(f_shard), s_one, w_in, w_out, mid, want_out=False, keep=True)
            if mlp_held is None:
                mlp_held = mlp_grads(plan.after(mid_slope), parts, dy_two, None, top, n_layers, None)
            f_in = later(f_in, mid_slope, mlp_held[0])
            f_back, attn_held, _ = attn_back(
                plan, f_in, d_one_bf, w_t, w_o2, mid + 1, n_heads, n_layers, attn_held
            )
            low_two = own(s_two) - finish((f_in,), (f_back,))
            mid_two = d_two + rms_pull(x_two_shard, scatter(f_back).astype(F32))
            d_two = mid_two + rms_pull(own(s_two), later(mid_sum, f_back).astype(F32))
            both_d = gather(jnp.stack([mid_two.astype(BF16), d_two.astype(BF16)], axis=1))
            dx, mid_dh = mlp_back_kept(plan, mid_slope, both_d, 0, w_in, w_out, mid)
            dx, low_dh = mlp_back_kept(plan, low_slope, both_d, 1, w_in, w_out, low, dx)
            dx_sum = scatter(dx)
            mid_parts, low_parts = (normed, mid_act, mid_dh), (normed, low_act, low_dh)
            mlp_held = mlp_grads(plan.after(dx), mid_parts, both_d, 0, mid, n_layers, mlp_held)
            x_two = ring_gather(later(low_two[0], both_d), (dx,), (mlp_held[0],))
            x_two_shard = low_two
            d_one = d_one + rms_pull(own(s_one), later(dx_sum, mlp_held[0]).astype(F32))
            heads, x_two = attn_forward(plan.after(d_one), x_two, w_t, low, n_heads)
            if layer_pair:
                d_shard, last = d_one.astype(BF16), dx
                g_sum, x_two_out = jnp.zeros_like(x_two_shard), x_two_shard
                mlp_held = mlp_grads(plan, low_parts, both_d, 1, low, n_layers, mlp_held)
        f_back, attn_held, d_one_full = attn_back(
            plan, x_two, gather(d_one, heads), w_t, w_o2, 0, n_heads, n_layers, attn_held, True
        )
        heads_all = gather(later(heads, d_one), f_back)
        d_two = d_two + rms_pull(x_two_shard, scatter(later(f_back, heads_all)).astype(F32))
        tail = plan.after(f_back)
        mlp_held = mlp_grads(tail, low_parts, both_d, 1, 0, n_layers, mlp_held)
        x_one = project_out(tail, s_one, heads_all, wo_all)
        d_two_full = gather(d_two, x_one, mlp_held[0])
        d_w = jnp.transpose(attn_held[0].reshape(n_layers, 3, n_heads, size, width), (0, 4, 1, 2, 3))
        d_wo = attn_held[1].reshape(n_layers, n_heads, size, width)
        return (x_one, x_two, d_one_full, d_two_full, d_w, d_wo) + tuple(mlp_held)

    return jax.shard_map(
        per_device,
        mesh=mesh,
        in_specs=(act_spec,) * 4 + (saved_spec,) * 2 + weight_specs,
        out_specs=(act_spec,) * 4 + grad_specs,
        check_vma=False,
    )
```
